256 devices in a mesh: sph: 256 (over x, y, z, core).
Axes of the slice: x: 4, y: 4, z: 8, core: 2. Of those that a mesh axis runs over, the one named last changes fastest.
Arguments:
- right_side: float32 [4096, 2, 336], P('sph'), may hold values from -8 to 8
- positions: float32 [3, 4096], P(None, 'sph'), may hold values from -0.1 to 15.1, as said below
- sphere_radii: float32 [4096], P('sph'), may hold values from 0.2 to 0.35
- azimuths: float32 [4096], P('sph'), may hold values from -3.1416 to 3.1416
- pair_flags: int32 [4096, 4096], P('sph'), may hold values from 0 to 2, as said below
- pair_counts: int32 [4096], P('sph'), may hold values from 1 to 4095, as said below
- tilt_matrix: float32 [336, 336], replicated, may hold values from -1 to 1
- axial_terms: float32 [8, 336, 336], replicated, may hold values from -1 to 1
Outputs:
- solution: float32 [4096, 2, 336], P('sph')
- residual: float32 [4096, 2, 336], P('sph')
- direction: float32 [4096, 2, 336], P('sph')
The draws below stay inside these ranges and needn't reach their ends.
Inputs may be any that keep to these rules, and one draw needn't show every extreme that they name: pair_flags is symmetric and zero on the diagonal. pair_counts[i] is the number of j with pair_flags[i, j] != 0; one sphere is linked to every other. `positions`: any two sphere centres are at least 0.8 apart.
All inputs are finite; a program needn't handle non-finite values.
Results may differ from the reference program's by a relative error of at most 0.0003.
Values sent between devices are 32-bit elements; how exact they have to be, the bound alone decides.
A program may use at most 64 MiB of HBM per device.

```python
import math
import jax
import jax.numpy as jnp
import numpy as np
from jax import lax

SPH_DEV = 16
DEG = 12
HALF = 168
C = 336
TERMS = 8
SPHERES = 4096
N_SPH = 256


def lattice_cells(total):
    sphere_ids = jnp.arange(total, dtype=jnp.int32)
    return jnp.stack([sphere_ids % 16, sphere_ids // 16 % 16, sphere_ids // 256])


def flag_table(key):
    cells = lattice_cells(SPHERES)
    spread = jnp.zeros((SPHERES, SPHERES), jnp.int32)
    for axis_index in range(3):
        spread = jnp.maximum(spread, jnp.abs(cells[axis_index][:, None] - cells[axis_index][None, :]))
    coin_bits = jax.random.randint(jax.random.fold_in(key, 11), (SPHERES, SPHERES), 0, 4)
    hub_sphere = jax.random.randint(jax.random.fold_in(key, 13), (), 0, SPHERES)
    row_ids = jnp.arange(SPHERES, dtype=jnp.int32)[:, None]
    col_ids = jnp.arange(SPHERES, dtype=jnp.int32)[None, :]
    shared_bits = jnp.where(row_ids < col_ids, coin_bits, coin_bits.T)
    hub_pair = (row_ids == hub_sphere) | (col_ids == hub_sphere)
    dropped = (shared_bits == 0) & jnp.logical_not(hub_pair) | (row_ids == col_ids)
    classes = jnp.where(spread <= 2, 1, 2)
    return jnp.where(dropped, 0, classes).astype(jnp.int32)


def draw_positions(key, part):
    cells = lattice_cells(SPHERES).astype(jnp.float32)
    jitter = jax.random.uniform(key, (3, SPHERES), jnp.float32, -0.1, 0.1)
    return cells + jitter


def draw_pair_flags(key, part):
    return flag_table(key)


def draw_pair_counts(key, part):
    return jnp.sum((flag_table(key) != 0).astype(jnp.int32), axis=1)


def scaled_matrix(key, shape, fan_width):
    values = jnp.clip(jax.random.normal(key, shape, jnp.float32), -4.0, 4.0) / math.sqrt(float(fan_width))
    return values


def draw_tilt_matrix(key, part):
    return scaled_matrix(jax.random.fold_in(key, 31), (C, C), C)


def draw_axial_terms(key, part):
    return scaled_matrix(jax.random.fold_in(key, 37), (TERMS, C, C), C)


def draw_azimuths(key, part):
    return jax.random.uniform(jax.random.fold_in(key, 41), (SPHERES,), jnp.float32, -math.pi, math.pi)


def orders_list():
    return np.concatenate([np.arange(-degree, degree + 1) for degree in range(1, DEG + 1)]).astype(np.float32)


def turn_rows(vector, azimuth, handed):
    phases = azimuth[:, None] * jnp.asarray(orders_list())[None, :]
    cosine = jnp.cos(phases)[:, None, :]
    sine_part = handed * jnp.sin(phases)[:, None, :]
    real_part = vector[..., :HALF]
    imag_part = vector[..., HALF:]
    return jnp.concatenate([cosine * real_part - sine_part * imag_part, sine_part * real_part + cosine * imag_part], axis=-1)


def leading_image(rough, key, part):
    centres = draw_positions(key, part)
    flags = flag_table(key)
    counts = jnp.sum((flags != 0).astype(jnp.float32), axis=1)
    angles = draw_azimuths(key, part)
    tilt = draw_tilt_matrix(key, part)
    axial_zero = draw_axial_terms(key, part)[0]
    delta = centres[:, :, None] - centres[:, None, :]
    distance = jnp.sqrt(jnp.sum(delta * delta, axis=0))
    weights = 0.25 * jnp.cos(2.5 * distance) * (flags != 0).astype(jnp.float32)
    framed = jnp.einsum('spk,kl->spl', turn_rows(rough, angles, 1.0), tilt, precision=lax.Precision.HIGHEST)
    summed = jnp.einsum('ij,jpk->ipk', weights, framed, precision=lax.Precision.HIGHEST)
    moved = jnp.einsum('ipk,kl->ipl', summed, axial_zero, precision=lax.Precision.HIGHEST)
    unturned = jnp.einsum('ipl,kl->ipk', moved, tilt, precision=lax.Precision.HIGHEST)
    unturned = unturned / jnp.sqrt(1.0 + counts)[:, None, None]
    return turn_rows(unturned, angles, -1.0)


def draw_right_side(key, part):
    rough = jnp.clip(jax.random.normal(jax.random.fold_in(key, 21), (SPHERES, 2, C), jnp.float32), -4.0, 4.0)
    return jnp.clip(rough + 2.0 * leading_image(rough, key, part), -8.0, 8.0)


def block_scale(own_key, extent, shards, least, top_value):
    level = 1.0
    for position, blocks in shards:
        steps = jax.random.uniform(jax.random.fold_in(jax.random.fold_in(own_key, 6), position), (blocks,), jnp.float32, least / len(shards), top_value / len(shards))
        level = level * jnp.repeat(jnp.exp(steps), extent[position] // blocks).reshape((-1,) + (1,) * (len(extent) - 1 - position))
    return level


def setup_inputs(seed: int = 0) -> dict:
    keys = jax.random.split(jax.random.key(seed), 9)
    return {
        "right_side": draw_right_side(jax.random.fold_in(keys[8], 71), 0),
        "positions": draw_positions(jax.random.fold_in(keys[8], 71), 0),
        "sphere_radii": jnp.clip(0.2 + 0.14999999 * jax.random.uniform(keys[2], (SPHERES,), jnp.float32) ** block_scale(keys[2], (SPHERES,), ((0, 256),), -0.2, 0.2), 0.2, 0.35),
        "azimuths": draw_azimuths(jax.random.fold_in(keys[8], 71), 0),
        "pair_flags": draw_pair_flags(jax.random.fold_in(keys[8], 71), 0),
        "pair_counts": draw_pair_counts(jax.random.fold_in(keys[8], 71), 0),
        "tilt_matrix": draw_tilt_matrix(jax.random.fold_in(keys[8], 71), 0),
        "axial_terms": draw_axial_terms(jax.random.fold_in(keys[8], 71), 0),
    }


coupling = 0.25
wavenum = 2.5
phase_step = 0.9
dist_floor = 0.8

def orders_table():
    return np.concatenate([np.arange(-degree, degree + 1) for degree in range(1, DEG + 1)]).astype(np.float32)

def rotate_z(vector, azimuth, handed):
    half_len = vector.shape[-1] // 2
    phases = azimuth[:, None] * jnp.asarray(orders_table())[None, :]
    cosine = jnp.cos(phases)[:, None, :]
    sine_part = handed * jnp.sin(phases)[:, None, :]
    real_part = vector[..., :half_len]
    imag_part = vector[..., half_len:]
    return jnp.concatenate([cosine * real_part - sine_part * imag_part, sine_part * real_part + cosine * imag_part], axis=-1)

def pair_weights(flag_block, geo_rows, geo_cols):
    delta_x = geo_rows[0][:, None] - geo_cols[0][None, :]
    delta_y = geo_rows[1][:, None] - geo_cols[1][None, :]
    delta_z = geo_rows[2][:, None] - geo_cols[2][None, :]
    distance = jnp.sqrt(delta_x * delta_x + delta_y * delta_y + delta_z * delta_z)
    size_ratio = (geo_rows[3][:, None] + geo_cols[3][None, :]) / jnp.maximum(distance, dist_floor)
    linked = (flag_block != 0).astype(distance.dtype)
    nearby = (flag_block == 1).astype(distance.dtype)
    ratio_power = jnp.ones_like(distance)
    weights = []
    for term_index in range(TERMS):
        selector = linked if term_index == 0 else nearby
        weights.append(coupling * ratio_power * jnp.cos(wavenum * distance + phase_step * term_index) * selector)
        ratio_power = ratio_power * size_ratio
    return jnp.stack(weights)

def to_frame(vector, azimuths, tilt_matrix):
    return jnp.einsum('spk,kl->spl', rotate_z(vector, azimuths, 1.0), tilt_matrix, precision=lax.Precision.HIGHEST)

def from_frame(coupled, azimuths, tilt_matrix, pair_counts):
    unturned = jnp.einsum('spl,kl->spk', coupled, tilt_matrix, precision=lax.Precision.HIGHEST)
    inverse_root = 1.0 / jnp.sqrt(1.0 + pair_counts.astype(jnp.float32))
    return rotate_z(unturned * inverse_root[:, None, None], azimuths, -1.0)

def operate(vector, azimuths, geometry, pair_flags, pair_counts, tilt_matrix, axial_terms):
    framed = to_frame(vector, azimuths, tilt_matrix)
    flat_rows = framed.reshape(SPHERES, -1)

    def target_block(block_index):
        row_start = block_index * SPH_DEV
        geo_rows = lax.dynamic_slice_in_dim(geometry, row_start, SPH_DEV, 1)
        flag_block = lax.dynamic_slice_in_dim(pair_flags, row_start, SPH_DEV, 0)
        weights = pair_weights(flag_block, geo_rows, geometry)
        gathered = jnp.einsum('mtj,jk->mtk', weights, flat_rows, precision=lax.Precision.HIGHEST)
        gathered = gathered.reshape(TERMS, SPH_DEV, 2, -1)
        return jnp.einsum('mtpk,mkl->tpl', gathered, axial_terms, precision=lax.Precision.HIGHEST)
    coupled = lax.map(target_block, jnp.arange(N_SPH, dtype=jnp.int32)).reshape(vector.shape)
    return vector - from_frame(coupled, azimuths, tilt_matrix, pair_counts)

def reference(right_side, positions, sphere_radii, azimuths, pair_flags, pair_counts, tilt_matrix, axial_terms):
    geometry = jnp.concatenate([positions, sphere_radii[None, :]], axis=0)

    def apply_op(vector):
        return operate(vector, azimuths, geometry, pair_flags, pair_counts, tilt_matrix, axial_terms)
    rho_start = jnp.sum(right_side * right_side)
    image_p = apply_op(right_side)
    step_alpha = rho_start / jnp.sum(right_side * image_p)
    half_step = right_side - step_alpha * image_p
    half_image = apply_op(half_step)
    step_omega = jnp.sum(half_image * half_step) / jnp.sum(half_image * half_image)
    solution = step_alpha * right_side + step_omega * half_step
    residual = half_step - step_omega * half_image
    rho_next = jnp.sum(right_side * residual)
    step_beta = rho_next / rho_start * (step_alpha / step_omega)
    direction = residual + step_beta * (right_side - step_omega * image_p)
    return (solution, residual, direction)
```

```python
import functools

import jax
import jax.numpy as jnp
import numpy as np
from jax import lax
from jax.experimental import pallas as pl
from jax.experimental.pallas import tpu as pltpu
from jax.sharding import Mesh
from jax.sharding import PartitionSpec as P

DEG = 12
TERMS = 8
SPH = ("sph_0", "sph_1", "sph_2", "sph_3")
NX, NY, NZ, NC = 4, 4, 8, 2
MESH = pl.DeviceIdType.MESH

coupling = 0.25
wavenum = 2.5
phase_step = 0.9
dist_floor = 0.8

SD = 16
HALF = 168
C = 336
CP = 384
LINE = NX * NY
SRC = LINE * NC * SD
TGT = NZ * SD
BF = jnp.bfloat16
F32 = jnp.float32


def orders_rows():
    orders = np.concatenate([np.arange(-degree, degree + 1) for degree in range(1, DEG + 1)])
    rows = np.zeros((8, CP), np.float32)
    rows[0, :HALF] = orders
    rows[0, HALF:C] = orders
    rows[1, :HALF] = 1.0
    rows[1, HALF:C] = -1.0
    return rows


def sincos(x):
    q = jnp.floor(x * (2.0 / np.pi) + 0.5)
    r = x - q * 1.5703125
    r = r - q * 4.83751296997070312e-4
    r = r - q * 7.54978995489188216e-8
    r2 = r * r
    s = r + r * r2 * (-1.6666654611e-1 + r2 * (8.3321608736e-3 + r2 * (-1.9515295891e-4)))
    c = 1.0 - 0.5 * r2 + r2 * r2 * (
        4.166664568298827e-2 + r2 * (-1.388731625493765e-3 + r2 * 2.443315711809948e-5)
    )
    quad = q - 4.0 * jnp.floor(q * 0.25)
    odd = (quad == 1.0) | (quad == 3.0)
    sin_sign = jnp.where(quad >= 2.0, -1.0, 1.0)
    cos_sign = jnp.where((quad == 1.0) | (quad == 2.0), -1.0, 1.0)
    return jnp.where(odd, c, s) * sin_sign, jnp.where(odd, s, c) * cos_sign


def split(x):
    high = x.astype(BF)
    return high, (x - high.astype(F32)).astype(BF)


def dot(a, b):
    return lax.dot_general(a, b, (((1,), (0,)), ((), ())), preferred_element_type=F32)


def dot_nt(a, b):
    return lax.dot_general(a, b, (((1,), (1,)), ((), ())), preferred_element_type=F32)


def lanes_of(x):
    total = jnp.sum(x, axis=0, keepdims=True)
    return total[:, 0:128] + total[:, 128:256] + total[:, 256:384]


def kernel(
    vec_ref, pos_ref, rad_ref, az_ref, flags_ref, counts_ref, tilt_ref, axial_hbm, rows_ref,
    sol_ref, res_ref, dir_ref,
    axial, ax_hi, ax_lo, tilt_hi, tilt_lo, flag_out, flag_in, mine, geo_src_out, geo_tgt_out,
    geo_src, geo_tgt, w_hi, w_lo, field, f_hi, f_lo, g_lhs, part, got, vec, img, img2,
    scal_out, scal_a, scal_mid, scal_b,
    ax_sem, geo_src_send, geo_src_recv, geo_tgt_send, geo_tgt_recv, flag_send, flag_recv,
    field_send, field_recv, pair_send, pair_recv, part_send, part_recv,
    sa_send, sa_recv, sb_send, sb_recv,
):
    mx, my, mz, mc = (lax.axis_index(name) for name in SPH)
    plane = mx * NY + my
    slot = plane * NC + mc

    def plane_peer(i):
        return (lax.rem(mx + i // NY, NX), lax.rem(my + lax.rem(i, NY), NY), mz, mc)

    def plane_source(i):
        return lax.rem(mx + NX - i // NY, NX) * NY + lax.rem(my + NY - lax.rem(i, NY), NY)

    def line_peer(j):
        return (mx, my, lax.rem(mz + j, NZ), mc)

    def pillar_peer(j):
        return (mx, my, lax.rem(mz + j // NC, NZ), lax.rem(mc + lax.rem(j, NC), NC))

    partner = (mx, my, mz, 1 - mc)

    def remote(src, dst, send, recv, peer):
        return pltpu.make_async_remote_copy(
            src_ref=src, dst_ref=dst, send_sem=send, recv_sem=recv, device_id=peer,
            device_id_type=MESH,
        )

    ax_copy = pltpu.make_async_copy(axial_hbm, axial, ax_sem)
    ax_copy.start()

    barrier = pltpu.get_barrier_semaphore()

    def greet_plane(i, carry):
        for core in range(NC):
            peer = plane_peer(i)
            pl.semaphore_signal(
                barrier, inc=1, device_id=(peer[0], peer[1], peer[2], core), device_id_type=MESH
            )
        return carry

    lax.fori_loop(1, LINE, greet_plane, 0)

    def greet_pillar(j, carry):
        pl.semaphore_signal(barrier, inc=1, device_id=pillar_peer(j), device_id_type=MESH)
        return carry

    lax.fori_loop(1, NZ * NC, greet_pillar, 0)

    mine[...] = jnp.zeros((8, 128), F32)
    mine[0:3, 0:SD] = pos_ref[...]
    mine[3:4, 0:SD] = rad_ref[...]
    mine[4:5, 0:SD] = az_ref[...]
    mine[5:6, 0:SD] = counts_ref[...].astype(F32)
    own = mine[...]
    lane = lax.broadcasted_iota(jnp.int32, (8, 128), 1)
    spread = own
    for shift in (16, 32, 64):
        spread = spread + pltpu.roll(spread, shift, 1)
    geo_src_out[...] = jnp.where(lane // SD == lax.rem(slot, 8), spread, 0.0)
    geo_tgt_out[...] = jnp.where(lane // SD == mz, spread, 0.0)
    geo_src[pl.ds(slot, 1)] = geo_src_out[...][None]
    geo_tgt[pl.ds(0, 1)] = geo_tgt_out[...][None]

    for z in range(NZ):
        r = z % 4
        for j in range(4):
            tile = None
            for i in range(4):
                at = ((4 * j + i) * 2 + z // 4) * 128
                piece = flags_ref[:, at : at + 128]
                if i != r:
                    piece = pltpu.roll(piece, (32 * (i - r)) % 128, 1)
                if tile is None:
                    tile = piece
                else:
                    where = lax.broadcasted_iota(jnp.int32, (SD, 128), 1) // 32 == i
                    tile = jnp.where(where, piece, tile)
            flag_out[z, :, 128 * j : 128 * (j + 1)] = tile

    cols = jnp.transpose(jnp.concatenate([own] * 16, axis=0))
    azimuth = cols[0:SD, 4:5]
    root = 1.0 / jnp.sqrt(1.0 + cols[0:SD, 5:6])
    sin_az, cos_az = sincos(azimuth * rows_ref[0:1, :])
    sin_az = sin_az * rows_ref[1:2, :]
    zeros_pad = jnp.zeros((CP - C, CP), BF)
    for half in range(2):
        for which, ref in enumerate((tilt_hi, tilt_lo)):
            ref[half * CP + C : half * CP + CP, :] = zeros_pad
    for half, (a, b) in enumerate(((0, HALF), (HALF, 0))):
        block = jnp.concatenate(
            [tilt_ref[a : a + HALF, :], tilt_ref[b : b + HALF, :]], axis=0
        )
        block = jnp.concatenate([block, jnp.zeros((C, CP - C), F32)], axis=1)
        high, low = split(block)
        tilt_hi[half * CP : half * CP + C, :] = high
        tilt_lo[half * CP : half * CP + C, :] = low

    def to_frame(x):
        high, low = split(jnp.concatenate([x * cos_az, x * sin_az], axis=1))
        both = dot(jnp.concatenate([high, low], axis=0), tilt_hi[...])
        return both[0:SD] + both[SD : 2 * SD] + dot(high, tilt_lo[...])

    def from_frame(x):
        high, low = split(x)
        both = dot_nt(jnp.concatenate([high, low], axis=0), tilt_hi[...])
        u = both[0:SD] + both[SD : 2 * SD] + dot_nt(high, tilt_lo[...])
        return (u[:, 0:CP] * cos_az + u[:, CP : 2 * CP] * sin_az) * root

    my_rows = pl.ds(pl.multiple_of(slot * SD, SD), SD)
    for h in range(2):
        v = jnp.concatenate([vec_ref[:, h, :], jnp.zeros((SD, CP - C), F32)], axis=1)
        vec[h] = v
        field[0, h, my_rows, :] = to_frame(v)

    pl.semaphore_wait(barrier, 2 * (LINE - 1) + NZ * NC - 1)

    def src_copy(i):
        peer = plane_peer(i // NC)
        peer = (peer[0], peer[1], mz, lax.rem(mc + lax.rem(i, NC), NC))
        return remote(geo_src_out, geo_src.at[slot], geo_src_send.at[i], geo_src_recv.at[i], peer)

    def tgt_copy(j):
        return remote(
            geo_tgt_out, geo_tgt.at[j], geo_tgt_send.at[j], geo_tgt_recv.at[j], line_peer(j)
        )

    def flag_copy(j):
        to = lax.rem(mz + j, NZ)
        return remote(
            flag_out.at[to], flag_in.at[j], flag_send.at[j], flag_recv.at[j], line_peer(j)
        )

    def field_copy(a, h, i):
        at = field.at[a, h, my_rows, :]
        return remote(at, at, field_send.at[a, h, i], field_recv.at[a, h, i], plane_peer(i))

    def pair_copy(a, h, i):
        rows = pl.ds(pl.multiple_of((plane_source(i) * NC + mc) * SD, SD), SD)
        at = field.at[a, h, rows, :]
        return remote(at, at, pair_send.at[a, h, i], pair_recv.at[a, h, i], partner)

    def part_copy(a, h, j):
        to = pl.ds(pl.multiple_of(lax.rem(mz + j, NZ) * SD, SD), SD)
        return remote(
            part.at[a, h, to, :], got.at[a, h, j], part_send.at[a, h, j], part_recv.at[a, h, j],
            line_peer(j),
        )

    def sa_copy(r, j):
        return remote(
            scal_out.at[r], scal_a.at[r, j], sa_send.at[r, j], sa_recv.at[r, j], pillar_peer(j)
        )

    def sb_copy(r, i):
        return remote(
            scal_mid.at[r], scal_b.at[r, i], sb_send.at[r, i], sb_recv.at[r, i], plane_peer(i)
        )

    def every(lo, hi, step):
        def body(k, carry):
            step(k)
            return carry

        lax.fori_loop(lo, hi, body, 0)

    def send_field(a, h):
        every(1, LINE, lambda i: field_copy(a, h, i).start())
        pair_copy(a, h, 0).start()

    every(1, LINE * NC, lambda i: src_copy(i).start())
    every(1, NZ, lambda j: tgt_copy(j).start())
    every(1, NZ, lambda j: flag_copy(j).start())
    send_field(0, 0)
    send_field(0, 1)

    ax_copy.wait()
    for m in range(TERMS):
        block = jnp.concatenate([axial[m], jnp.zeros((C, CP - C), F32)], axis=1)
        high, low = split(block)
        for ref, value in ((ax_hi, high), (ax_lo, low)):
            ref[m * CP : m * CP + C, :] = value
            ref[m * CP + C : (m + 1) * CP, :] = zeros_pad

    every(1, LINE * NC, lambda i: src_copy(i).wait_recv())
    every(1, NZ, lambda j: tgt_copy(j).wait_recv())
    src_rows = []
    for tile in range(SRC // 128):
        total = geo_src[8 * tile]
        for k in range(1, 8):
            total = total + geo_src[8 * tile + k]
        src_rows.append(total)
    src_all = jnp.concatenate(src_rows, axis=1)
    tgt_all = geo_tgt[0]
    for j in range(1, NZ):
        tgt_all = tgt_all + geo_tgt[j]
    mine[...] = tgt_all
    geo_cols = jnp.transpose(jnp.concatenate([tgt_all] * 16, axis=0))
    geo_col_ref = g_col = None
    del geo_col_ref, g_col
    part[0, 0, :, 0:128] = geo_cols

    def weigh(flags, z):
        rows = pl.ds(pl.multiple_of(z * SD, SD), SD)
        tgt = part[0, 0, rows, 0:128]
        dx = tgt[:, 0:1] - src_all[0:1, :]
        dy = tgt[:, 1:2] - src_all[1:2, :]
        dz = tgt[:, 2:3] - src_all[2:3, :]
        dist = jnp.sqrt(dx * dx + dy * dy + dz * dz)
        ratio = (tgt[:, 3:4] + src_all[3:4, :]) / jnp.maximum(dist, dist_floor)
        sin_d, cos_d = sincos(wavenum * dist)
        scale = jnp.where(flags != 0, coupling, 0.0)
        near = jnp.where(flags == 1, coupling, 0.0)
        for m in range(TERMS):
            if m > 0:
                near = near * ratio
                scale = near
            wave = cos_d * float(np.cos(phase_step * m)) - sin_d * float(np.sin(phase_step * m))
            high, low = split(wave * scale)
            at = pl.ds(pl.multiple_of(m * TGT + z * SD, SD), SD)
            w_hi[at, :] = high
            w_lo[at, :] = low

    weigh(flag_out[mz], mz)

    def weigh_from(j, carry):
        flag_copy(j).wait_recv()
        weigh(flag_in[j], lax.rem(mz + NZ - j, NZ))
        return carry

    lax.fori_loop(1, NZ, weigh_from, 0)

    def couple(a, h):
        def relay(i):
            field_copy(a, h, i).wait_recv()
            pair_copy(a, h, i).start()

        every(1, LINE, relay)
        every(0, LINE, lambda i: pair_copy(a, h, i).wait_recv())
        high, low = split(field[a, h])
        f_hi[...] = high
        f_lo[...] = low
        for block in range(2):
            at = slice(block * 512, (block + 1) * 512)
            g = dot(w_hi[at, :], f_hi[...]) + dot(w_hi[at, :], f_lo[...]) + dot(w_lo[at, :], f_hi[...])
            g_high, g_low = split(g)
            for k in range(4):
                m = block * 4 + k
                g_lhs[0:TGT, m * CP : (m + 1) * CP] = g_high[k * TGT : (k + 1) * TGT]
                g_lhs[TGT : 2 * TGT, m * CP : (m + 1) * CP] = g_low[k * TGT : (k + 1) * TGT]
        both = dot(g_lhs[...], ax_hi[...])
        part[a, h] = both[0:TGT] + both[TGT : 2 * TGT] + dot(g_lhs[0:TGT, :], ax_lo[...])
        every(1, NZ, lambda j: part_copy(a, h, j).start())

    def collect(a, h):
        total = part[a, h, pl.ds(pl.multiple_of(mz * SD, SD), SD), :]
        every(1, NZ, lambda j: part_copy(a, h, j).wait_recv())
        for j in range(1, NZ):
            total = total + got[a, h, j]
        return from_frame(total)

    def reduce_pillar(r):
        every(1, NZ * NC, lambda j: sa_copy(r, j).wait_recv())
        total = scal_out[r]
        for j in range(1, NZ * NC):
            total = total + scal_a[r, j]
        scal_mid[r] = total
        every(1, LINE, lambda i: sb_copy(r, i).start())

    def reduce_plane(r):
        every(1, LINE, lambda i: sb_copy(r, i).wait_recv())
        total = scal_mid[r]
        for i in range(1, LINE):
            total = total + scal_b[r, i]
        return jnp.sum(total, axis=1, keepdims=True)

    couple(0, 0)
    couple(0, 1)
    for h in range(2):
        image = vec[h] - collect(0, h)
        img[h] = image
        field[1, h, my_rows, :] = to_frame(image)
        send_field(1, h)

    scal_out[...] = jnp.zeros((2, 8, 128), F32)
    scal_out[0, 0:1, :] = lanes_of(vec[0] * vec[0] + vec[1] * vec[1])
    scal_out[0, 1:2, :] = lanes_of(vec[0] * img[0] + vec[1] * img[1])
    every(1, NZ * NC, lambda j: sa_copy(0, j).start())
    couple(1, 0)
    reduce_pillar(0)
    couple(1, 1)
    sums = reduce_plane(0)
    rho_start = sums[0:1, :]
    alpha = rho_start / sums[1:2, :]

    def inner(left, right):
        return lanes_of(left[0] * right[0] + left[1] * right[1])

    half_step = []
    half_image = []
    for h in range(2):
        image = img[h]
        second = image - collect(1, h)
        half_step.append(vec[h] - alpha * image)
        half_image.append(image - alpha * second)
    right = [vec[0], vec[1]]
    scal_out[1, 0:1, :] = inner(half_image, half_step)
    scal_out[1, 1:2, :] = inner(half_image, half_image)
    scal_out[1, 2:3, :] = inner(right, half_step)
    scal_out[1, 3:4, :] = inner(right, half_image)
    every(1, NZ * NC, lambda j: sa_copy(1, j).start())
    reduce_pillar(1)
    sums = reduce_plane(1)
    omega = sums[0:1, :] / sums[1:2, :]
    rho_next = sums[2:3, :] - omega * sums[3:4, :]
    beta = rho_next / rho_start * (alpha / omega)
    for h in range(2):
        res = half_step[h] - omega * half_image[h]
        sol_ref[:, h, :] = (alpha * right[h] + omega * half_step[h])[:, 0:C]
        res_ref[:, h, :] = res[:, 0:C]
        dir_ref[:, h, :] = (res + beta * (right[h] - omega * img[h]))[:, 0:C]

    every(1, LINE * NC, lambda i: src_copy(i).wait_send())
    every(1, NZ, lambda j: tgt_copy(j).wait_send())
    every(1, NZ, lambda j: flag_copy(j).wait_send())
    for a in range(2):
        for h in range(2):
            every(1, LINE, lambda i: field_copy(a, h, i).wait_send())
            every(0, LINE, lambda i: pair_copy(a, h, i).wait_send())
            every(1, NZ, lambda j: part_copy(a, h, j).wait_send())
        every(1, NZ * NC, lambda j: sa_copy(a, j).wait_send())
        every(1, LINE, lambda i: sb_copy(a, i).wait_send())


def on_device(
    right_side, positions, sphere_radii, azimuths, pair_flags, pair_counts, tilt_matrix, axial_terms
):
    vmem = pl.BlockSpec(memory_space=pltpu.VMEM)
    hbm = pl.BlockSpec(memory_space=pl.ANY)
    dma = pltpu.SemaphoreType.DMA
    out = jax.ShapeDtypeStruct((SD, 2, C), F32)
    V = pltpu.VMEM
    return tuple(
        pl.pallas_call(
            kernel,
            name="bicgstab",
            out_shape=(out, out, out),
            in_specs=[vmem] * 7 + [hbm, vmem],
            out_specs=(vmem, vmem, vmem),
            scratch_shapes=[
                V((TERMS, C, C), F32),
                V((TERMS * CP, CP), BF),
                V((TERMS * CP, CP), BF),
                V((2 * CP, CP), BF),
                V((2 * CP, CP), BF),
                V((NZ, SD, SRC), jnp.int32),
                V((NZ, SD, SRC), jnp.int32),
                V((8, 128), F32),
                V((8, 128), F32),
                V((8, 128), F32),
                V((LINE * NC, 8, 128), F32),
                V((NZ, 8, 128), F32),
                V((TERMS * TGT, SRC), BF),
                V((TERMS * TGT, SRC), BF),
                V((2, 2, SRC, CP), F32),
                V((SRC, CP), BF),
                V((SRC, CP), BF),
                V((2 * TGT, TERMS * CP), BF),
                V((2, 2, TGT, CP), F32),
                V((2, 2, NZ, SD, CP), F32),
                V((2, SD, CP), F32),
                V((2, SD, CP), F32),
                V((2, SD, CP), F32),
                V((2, 8, 128), F32),
                V((2, NZ * NC, 8, 128), F32),
                V((2, 8, 128), F32),
                V((2, LINE, 8, 128), F32),
                dma(()),
                dma((LINE * NC,)),
                dma((LINE * NC,)),
                dma((NZ,)),
                dma((NZ,)),
                dma((NZ,)),
                dma((NZ,)),
                dma((2, 2, LINE)),
                dma((2, 2, LINE)),
                dma((2, 2, LINE)),
                dma((2, 2, LINE)),
                dma((2, 2, NZ)),
                dma((2, 2, NZ)),
                dma((2, NZ * NC)),
                dma((2, NZ * NC)),
                dma((2, LINE)),
                dma((2, LINE)),
            ],
            compiler_params=pltpu.CompilerParams(
                collective_id=0, has_side_effects=True, vmem_limit_bytes=48 * 1024 * 1024
            ),
        )(
            right_side,
            positions,
            sphere_radii.reshape(1, SD),
            azimuths.reshape(1, SD),
            pair_flags,
            pair_counts.reshape(1, SD),
            tilt_matrix,
            axial_terms,
            jnp.asarray(orders_rows()),
        )
    )


def solution(mesh):
    split_mesh = Mesh(mesh.devices.reshape(NX, NY, NZ, NC), SPH)
    placed = (P(SPH, None, None), P(None, SPH), P(SPH), P(SPH), P(SPH, None), P(SPH), P(), P())
    return jax.shard_map(
        on_device,
        mesh=split_mesh,
        in_specs=placed,
        out_specs=(P(SPH, None, None), P(SPH, None, None), P(SPH, None, None)),
        check_vma=False,
    )
```

```python
import functools

import jax
import jax.numpy as jnp
import numpy as np
from jax import lax
from jax.experimental import pallas as pl
from jax.experimental.pallas import tpu as pltpu
from jax.sharding import Mesh
from jax.sharding import PartitionSpec as P

DEG = 12
TERMS = 8
SPH = ("sph_0", "sph_1", "sph_2", "sph_3")
NX, NY, NZ, NC = 4, 4, 8, 2
MESH = pl.DeviceIdType.MESH

coupling = 0.25
wavenum = 2.5
phase_step = 0.9
dist_floor = 0.8

SD = 16
HALF = 168
C = 336
CP = 384
LINE = NX * NY
SRC = LINE * NC * SD
TGT = NZ * SD
RINGS = (
    ((2, 2), (1, 2), (3, 2), (2, 1), (2, 3)),
    ((0, 2), (2, 0), (1, 1), (1, 3), (3, 1), (3, 3)),
    ((0, 1), (0, 3), (1, 0), (3, 0)),
)
LINE_ORDER = (4, 3, 5, 2, 6, 1, 7)
PLANE_ORDER = tuple(offset for ring in RINGS for offset in ring)
PILLAR_ORDER = tuple((j, core) for j in LINE_ORDER for core in (1, 0)) + ((0, 1),)
BF = jnp.bfloat16
F32 = jnp.float32


def orders_rows():
    orders = np.concatenate([np.arange(-degree, degree + 1) for degree in range(1, DEG + 1)])
    rows = np.zeros((8, CP), np.float32)
    rows[0, :HALF] = orders
    rows[0, HALF:C] = orders
    rows[1, :HALF] = 1.0
    rows[1, HALF:C] = -1.0
    return rows


def sincos(x):
    q = jnp.floor(x * (2.0 / np.pi) + 0.5)
    r = x - q * 1.5703125
    r = r - q * 4.83751296997070312e-4
    r = r - q * 7.54978995489188216e-8
    r2 = r * r
    s = r + r * r2 * (-1.6666654611e-1 + r2 * (8.3321608736e-3 + r2 * (-1.9515295891e-4)))
    c = 1.0 - 0.5 * r2 + r2 * r2 * (
        4.166664568298827e-2 + r2 * (-1.388731625493765e-3 + r2 * 2.443315711809948e-5)
    )
    quad = q - 4.0 * jnp.floor(q * 0.25)
    odd = (quad == 1.0) | (quad == 3.0)
    sin_sign = jnp.where(quad >= 2.0, -1.0, 1.0)
    cos_sign = jnp.where((quad == 1.0) | (quad == 2.0), -1.0, 1.0)
    return jnp.where(odd, c, s) * sin_sign, jnp.where(odd, s, c) * cos_sign


def split(x):
    high = x.astype(BF)
    return high, (x - high.astype(F32)).astype(BF)


def dot(a, b):
    return lax.dot_general(a, b, (((1,), (0,)), ((), ())), preferred_element_type=F32)


def dot_nt(a, b):
    return lax.dot_general(a, b, (((1,), (1,)), ((), ())), preferred_element_type=F32)


def lanes_of(x):
    total = jnp.sum(x, axis=0, keepdims=True)
    return total[:, 0:128] + total[:, 128:256] + total[:, 256:384]


def kernel(
    vec_hbm, pos_hbm, rad_hbm, az_hbm, flags_hbm, counts_hbm, tilt_hbm, axial_hbm, rows_hbm,
    sol_ref, res_ref, dir_ref,
    vec_ref, pos_ref, rad_ref, az_ref, flags_ref, counts_ref, tilt_ref, axial, rows_ref, ax_hi, ax_lo, tilt_hi, tilt_lo, flag_out, flag_in, mine, geo_src_out, geo_tgt_out,
    geo_src, geo_tgt, w_hi, w_lo, field, f_hi, f_lo, g_lhs, part, got, vec, img, img2,
    scal_out, scal_a, scal_mid, scal_b,
    in_sem, geo_src_send, geo_src_recv, geo_tgt_send, geo_tgt_recv, flag_send, flag_recv,
    field_send, field_recv, pair_send, pair_recv, part_send, part_recv,
    sa_send, sa_recv, sb_send, sb_recv,
):
    mx, my, mz, mc = (lax.axis_index(name) for name in SPH)
    plane = mx * NY + my
    slot = plane * NC + mc

    def plane_peer(offset, core):
        return (lax.rem(mx + offset[0], NX), lax.rem(my + offset[1], NY), mz, core)

    def line_peer(j):
        return (mx, my, lax.rem(mz + j, NZ), mc)

    def pillar_peer(j, core):
        return (mx, my, lax.rem(mz + j, NZ), mc if core == 0 else 1 - mc)

    partner = (mx, my, mz, 1 - mc)

    def remote(src, dst, send, recv, peer):
        return pltpu.make_async_remote_copy(
            src_ref=src, dst_ref=dst, send_sem=send, recv_sem=recv, device_id=peer,
            device_id_type=MESH,
        )

    with jax.named_scope("loads"):
        pairs = (
            (pos_hbm, pos_ref), (rad_hbm, rad_ref), (az_hbm, az_ref), (counts_hbm, counts_ref),
            (rows_hbm, rows_ref), (flags_hbm, flags_ref), (tilt_hbm, tilt_ref), (vec_hbm, vec_ref),
            (axial_hbm, axial),
        )
        loads = [pltpu.make_async_copy(a, b, in_sem.at[k]) for k, (a, b) in enumerate(pairs)]
        for load in loads:
            load.start()

        barrier = pltpu.get_barrier_semaphore()

        def greet(peer):
            pl.semaphore_signal(barrier, inc=1, device_id=peer, device_id_type=MESH)

        for j, core in PILLAR_ORDER:
            greet(pillar_peer(j, core))
        for offset in PLANE_ORDER:
            for core in range(NC):
                greet(plane_peer(offset, core))

        for load in loads[:6]:
            load.wait()

    with jax.named_scope("geo_prep"):
        mine[...] = jnp.zeros((8, 128), F32)
        mine[0:3, 0:SD] = pos_ref[...]
        mine[3:4, 0:SD] = rad_ref[...]
        mine[4:5, 0:SD] = az_ref[...]
        mine[5:6, 0:SD] = counts_ref[...].astype(F32)
        own = mine[...]
        lane = lax.broadcasted_iota(jnp.int32, (8, 128), 1)
        spread = own
        for shift in (16, 32, 64):
            spread = spread + pltpu.roll(spread, shift, 1)
        geo_src_out[...] = jnp.where(lane // SD == lax.rem(slot, 8), spread, 0.0)
        geo_tgt_out[...] = jnp.where(lane // SD == mz, spread, 0.0)
        geo_src[pl.ds(slot, 1)] = geo_src_out[...][None]
        geo_tgt[pl.ds(0, 1)] = geo_tgt_out[...][None]

    with jax.named_scope("flag_prep"):
        for z in range(NZ):
            r = z % 4
            for j in range(4):
                tile = None
                for i in range(4):
                    at = ((4 * j + i) * 2 + z // 4) * 128
                    piece = flags_ref[:, at : at + 128]
                    if i != r:
                        piece = pltpu.roll(piece, (32 * (i - r)) % 128, 1)
                    if tile is None:
                        tile = piece
                    else:
                        where = lax.broadcasted_iota(jnp.int32, (SD, 128), 1) // 32 == i
                        tile = jnp.where(where, piece, tile)
                flag_out[z, :, 128 * j : 128 * (j + 1)] = tile

    loads[6].wait()
    loads[7].wait()
    cols = jnp.transpose(jnp.concatenate([own] * 16, axis=0))
    azimuth = cols[0:SD, 4:5]
    root = 1.0 / jnp.sqrt(1.0 + cols[0:SD, 5:6])
    sin_az, cos_az = sincos(azimuth * rows_ref[0:1, :])
    sin_az = sin_az * rows_ref[1:2, :]
    zeros_pad = jnp.zeros((CP - C, CP), BF)
    for half in range(2):
        for which, ref in enumerate((tilt_hi, tilt_lo)):
            ref[half * CP + C : half * CP + CP, :] = zeros_pad
    for half, (a, b) in enumerate(((0, HALF), (HALF, 0))):
        block = jnp.concatenate(
            [tilt_ref[a : a + HALF, :], tilt_ref[b : b + HALF, :]], axis=0
        )
        block = jnp.concatenate([block, jnp.zeros((C, CP - C), F32)], axis=1)
        high, low = split(block)
        tilt_hi[half * CP : half * CP + C, :] = high
        tilt_lo[half * CP : half * CP + C, :] = low

    def to_frame(x):
        high, low = split(jnp.concatenate([x * cos_az, x * sin_az], axis=1))
        both = dot(jnp.concatenate([high, low], axis=0), tilt_hi[...])
        return both[0:SD] + both[SD : 2 * SD] + dot(high, tilt_lo[...])

    def from_frame(x):
        high, low = split(x)
        both = dot_nt(jnp.concatenate([high, low], axis=0), tilt_hi[...])
        u = both[0:SD] + both[SD : 2 * SD] + dot_nt(high, tilt_lo[...])
        return (u[:, 0:CP] * cos_az + u[:, CP : 2 * CP] * sin_az) * root

    my_rows = pl.ds(pl.multiple_of(slot * SD, SD), SD)
    with jax.named_scope("frame0"):
        for h in range(2):
            v = jnp.concatenate([vec_ref[:, h, :], jnp.zeros((SD, CP - C), F32)], axis=1)
            vec[h] = v
            field[0, h, my_rows, :] = to_frame(v)

    with jax.named_scope("barrier_wait"):
        pl.semaphore_wait(barrier, 2 * (LINE - 1) + NZ * NC - 1)

    def src_copy(peer):
        return remote(geo_src_out, geo_src.at[slot], geo_src_send, geo_src_recv, peer)

    src_all_copies = remote(
        geo_src.at[pl.ds(0, LINE * NC - 1)], geo_src.at[pl.ds(0, LINE * NC - 1)],
        geo_src_send, geo_src_recv, partner,
    )

    def tgt_copy(j):
        return remote(geo_tgt_out, geo_tgt.at[j], geo_tgt_send, geo_tgt_recv, line_peer(j))

    tgt_all_copies = remote(
        geo_tgt.at[pl.ds(0, NZ - 1)], geo_tgt.at[pl.ds(0, NZ - 1)],
        geo_tgt_send, geo_tgt_recv, partner,
    )

    def flag_copy(j):
        to = lax.rem(mz + j, NZ)
        return remote(flag_out.at[to], flag_in.at[j], flag_send, flag_recv.at[j], line_peer(j))

    def blocks(a, h, count, send, recv):
        at = field.at[a, h, pl.ds(0, count * SD), :]
        return remote(at, at, send, recv, partner)

    def field_copy(a, h, ring, offset):
        at = field.at[a, h, my_rows, :]
        return remote(
            at, at, field_send.at[a, h], field_recv.at[a, h, ring], plane_peer(offset, 1 - mc)
        )

    def pair_copy(a, h, offset):
        source = lax.rem(mx + NX - offset[0], NX) * NY + lax.rem(my + NY - offset[1], NY)
        core = mc if offset == (0, 0) else 1 - mc
        rows = pl.ds(pl.multiple_of((source * NC + core) * SD, SD), SD)
        at = field.at[a, h, rows, :]
        return remote(at, at, pair_send.at[a, h], pair_recv.at[a, h], partner)

    def send_part(a, h):
        for k, j in enumerate(LINE_ORDER):
            to = pl.ds(pl.multiple_of(lax.rem(mz + j, NZ) * SD, SD), SD)
            remote(
                part.at[a, h, to, :], got.at[a, h, k], part_send.at[a, h], part_recv.at[a, h],
                line_peer(j),
            ).start()

    def part_all(a, h):
        at = got.at[a, h, pl.ds(0, NZ - 1)]
        return remote(at, at, part_send.at[a, h], part_recv.at[a, h], partner)

    def send_pillar(r):
        for k, (j, core) in enumerate(PILLAR_ORDER):
            remote(
                scal_out.at[r], scal_a.at[r, k], sa_send.at[r], sa_recv.at[r], pillar_peer(j, core)
            ).start()

    def sa_all(r):
        at = scal_a.at[r, pl.ds(0, NZ * NC - 1)]
        return remote(at, at, sa_send.at[r], sa_recv.at[r], partner)

    def send_plane(r):
        for k, offset in enumerate(PLANE_ORDER):
            remote(
                scal_mid.at[r], scal_b.at[r, k], sb_send.at[r], sb_recv.at[r],
                plane_peer(offset, mc),
            ).start()

    def sb_all(r):
        at = scal_b.at[r, pl.ds(0, LINE - 1)]
        return remote(at, at, sb_send.at[r], sb_recv.at[r], partner)

    def send_field(a, h):
        for ring, offsets in enumerate(RINGS):
            for offset in offsets:
                field_copy(a, h, ring, offset).start()
        pair_copy(a, h, (0, 0)).start()

    def relay(a, h, ring):
        with jax.named_scope(f"relay{a}{h}{ring}"):
            blocks(a, h, len(RINGS[ring]), field_send.at[a, h], field_recv.at[a, h, ring]).wait_recv()
            for offset in RINGS[ring]:
                pair_copy(a, h, offset).start()

    with jax.named_scope("sends"):
        for offset in PLANE_ORDER:
            for core in range(NC):
                src_copy(plane_peer(offset, core)).start()
        src_copy(partner).start()
        for j in LINE_ORDER:
            tgt_copy(j).start()
        for j in LINE_ORDER:
            flag_copy(j).start()
        send_field(0, 0)
        send_field(0, 1)

    with jax.named_scope("axial"):
        loads[8].wait()
        for m in range(TERMS):
            block = jnp.concatenate([axial[m], jnp.zeros((C, CP - C), F32)], axis=1)
            high, low = split(block)
            for ref, value in ((ax_hi, high), (ax_lo, low)):
                ref[m * CP : m * CP + C, :] = value
                ref[m * CP + C : (m + 1) * CP, :] = zeros_pad

    with jax.named_scope("geo_wait"):
        src_all_copies.wait_recv()
        tgt_all_copies.wait_recv()
    src_rows = []
    for tile in range(SRC // 128):
        total = geo_src[8 * tile]
        for k in range(1, 8):
            total = total + geo_src[8 * tile + k]
        src_rows.append(total)
    src_all = jnp.concatenate(src_rows, axis=1)
    tgt_all = geo_tgt[0]
    for j in range(1, NZ):
        tgt_all = tgt_all + geo_tgt[j]
    part[0, 0, :, 0:128] = jnp.transpose(jnp.concatenate([tgt_all] * 16, axis=0))

    def weigh(flags, z):
        rows = pl.ds(pl.multiple_of(z * SD, SD), SD)
        tgt = part[0, 0, rows, 0:128]
        dx = tgt[:, 0:1] - src_all[0:1, :]
        dy = tgt[:, 1:2] - src_all[1:2, :]
        dz = tgt[:, 2:3] - src_all[2:3, :]
        dist = jnp.sqrt(dx * dx + dy * dy + dz * dz)
        ratio = (tgt[:, 3:4] + src_all[3:4, :]) / jnp.maximum(dist, dist_floor)
        sin_d, cos_d = sincos(wavenum * dist)
        scale = jnp.where(flags != 0, coupling, 0.0)
        near = jnp.where(flags == 1, coupling, 0.0)
        for m in range(TERMS):
            if m > 0:
                near = near * ratio
                scale = near
            wave = cos_d * float(np.cos(phase_step * m)) - sin_d * float(np.sin(phase_step * m))
            high, low = split(wave * scale)
            at = pl.ds(pl.multiple_of(m * TGT + z * SD, SD), SD)
            w_hi[at, :] = high
            w_lo[at, :] = low

    with jax.named_scope("weigh"):
        weigh(flag_out[mz], mz)

        def weigh_from(j, carry):
            flag_copy(j).wait_recv()
            weigh(flag_in[j], lax.rem(mz + NZ - j, NZ))
            return carry

        for ring, (lo, hi) in enumerate(((1, 5), (5, 7), (7, 8))):
            lax.fori_loop(lo, hi, weigh_from, 0)
            relay(0, 0, ring)

    def couple(a, h):
        with jax.named_scope(f"gather_wait{a}{h}"):
            blocks(a, h, LINE, pair_send.at[a, h], pair_recv.at[a, h]).wait_recv()
        with jax.named_scope(f"first{a}{h}"):
            high, low = split(field[a, h])
            f_hi[...] = high
            f_lo[...] = low
            for block in range(2):
                at = slice(block * 512, (block + 1) * 512)
                g = dot(w_hi[at, :], f_hi[...]) + dot(w_hi[at, :], f_lo[...]) + dot(w_lo[at, :], f_hi[...])
                g_high, g_low = split(g)
                for k in range(4):
                    m = block * 4 + k
                    g_lhs[0:TGT, m * CP : (m + 1) * CP] = g_high[k * TGT : (k + 1) * TGT]
                    g_lhs[TGT : 2 * TGT, m * CP : (m + 1) * CP] = g_low[k * TGT : (k + 1) * TGT]
        if h == 0:
            for ring in range(len(RINGS)):
                relay(a, 1, ring)
        with jax.named_scope(f"second{a}{h}"):
            both = dot(g_lhs[...], ax_hi[...])
            part[a, h] = both[0:TGT] + both[TGT : 2 * TGT] + dot(g_lhs[0:TGT, :], ax_lo[...])
            send_part(a, h)

    def collect(a, h):
        total = part[a, h, pl.ds(pl.multiple_of(mz * SD, SD), SD), :]
        with jax.named_scope(f"part_wait{a}{h}"):
            part_all(a, h).wait_recv()
        for k in range(NZ - 1):
            total = total + got[a, h, k]
        return from_frame(total)

    def reduce_pillar(r):
        with jax.named_scope(f"pillar_wait{r}"):
            sa_all(r).wait_recv()
        total = scal_out[r]
        for k in range(NZ * NC - 1):
            total = total + scal_a[r, k]
        scal_mid[r] = total
        send_plane(r)

    def reduce_plane(r):
        with jax.named_scope(f"plane_wait{r}"):
            sb_all(r).wait_recv()
        total = scal_mid[r]
        for k in range(LINE - 1):
            total = total + scal_b[r, k]
        return jnp.sum(total, axis=1, keepdims=True)

    couple(0, 0)
    couple(0, 1)
    for h in range(2):
        image = vec[h] - collect(0, h)
        img[h] = image
        field[1, h, my_rows, :] = to_frame(image)
        send_field(1, h)

    scal_out[...] = jnp.zeros((2, 8, 128), F32)
    scal_out[0, 0:1, :] = lanes_of(vec[0] * vec[0] + vec[1] * vec[1])
    scal_out[0, 1:2, :] = lanes_of(vec[0] * img[0] + vec[1] * img[1])
    send_pillar(0)
    for ring in range(len(RINGS)):
        relay(1, 0, ring)
    couple(1, 0)
    reduce_pillar(0)
    couple(1, 1)
    sums = reduce_plane(0)
    rho_start = sums[0:1, :]
    alpha = rho_start / sums[1:2, :]

    def inner(left, right):
        return lanes_of(left[0] * right[0] + left[1] * right[1])

    half_step = []
    half_image = []
    for h in range(2):
        image = img[h]
        second = image - collect(1, h)
        half_step.append(vec[h] - alpha * image)
        half_image.append(image - alpha * second)
    right = [vec[0], vec[1]]
    scal_out[1, 0:1, :] = inner(half_image, half_step)
    scal_out[1, 1:2, :] = inner(half_image, half_image)
    scal_out[1, 2:3, :] = inner(right, half_step)
    scal_out[1, 3:4, :] = inner(right, half_image)
    send_pillar(1)
    reduce_pillar(1)
    sums = reduce_plane(1)
    omega = sums[0:1, :] / sums[1:2, :]
    rho_next = sums[2:3, :] - omega * sums[3:4, :]
    beta = rho_next / rho_start * (alpha / omega)
    for h in range(2):
        res = half_step[h] - omega * half_image[h]
        sol_ref[:, h, :] = (alpha * right[h] + omega * half_step[h])[:, 0:C]
        res_ref[:, h, :] = res[:, 0:C]
        dir_ref[:, h, :] = (res + beta * (right[h] - omega * img[h]))[:, 0:C]

    with jax.named_scope("drain"):
        src_all_copies.wait_send()
        tgt_all_copies.wait_send()
        sent = flag_in.at[pl.ds(0, NZ - 1)]
        remote(sent, sent, flag_send, flag_recv.at[0], partner).wait_send()
        for a in range(2):
            for h in range(2):
                blocks(a, h, LINE - 1, field_send.at[a, h], field_recv.at[a, h, 0]).wait_send()
                blocks(a, h, LINE, pair_send.at[a, h], pair_recv.at[a, h]).wait_send()
                part_all(a, h).wait_send()
            sa_all(a).wait_send()
            sb_all(a).wait_send()


def put_out(*refs):
    for k in range(3):
        refs[3 + k][...] = refs[k][...]


def on_device(
    right_side, positions, sphere_radii, azimuths, pair_flags, pair_counts, tilt_matrix, axial_terms
):
    vmem = pl.BlockSpec(memory_space=pltpu.VMEM)
    hbm = pl.BlockSpec(memory_space=pltpu.HBM)
    dma = pltpu.SemaphoreType.DMA
    out = jax.ShapeDtypeStruct((SD, 2, C), F32)
    V = pltpu.VMEM
    results = tuple(
        pl.pallas_call(
            kernel,
            name="bicgstab",
            out_shape=(out, out, out),
            in_specs=[hbm] * 9,
            out_specs=(vmem, vmem, vmem),
            scratch_shapes=[
                V((SD, 2, C), F32),
                V((3, SD), F32),
                V((1, SD), F32),
                V((1, SD), F32),
                V((SD, LINE * NZ * NC * SD), jnp.int32),
                V((1, SD), jnp.int32),
                V((C, C), F32),
                V((TERMS, C, C), F32),
                V((8, CP), F32),
                V((TERMS * CP, CP), BF),
                V((TERMS * CP, CP), BF),
                V((2 * CP, CP), BF),
                V((2 * CP, CP), BF),
                V((NZ, SD, SRC), jnp.int32),
                V((NZ, SD, SRC), jnp.int32),
                V((8, 128), F32),
                V((8, 128), F32),
                V((8, 128), F32),
                V((LINE * NC, 8, 128), F32),
                V((NZ, 8, 128), F32),
                V((TERMS * TGT, SRC), BF),
                V((TERMS * TGT, SRC), BF),
                V((2, 2, SRC, CP), F32),
                V((SRC, CP), BF),
                V((SRC, CP), BF),
                V((2 * TGT, TERMS * CP), BF),
                V((2, 2, TGT, CP), F32),
                V((2, 2, NZ, SD, CP), F32),
                V((2, SD, CP), F32),
                V((2, SD, CP), F32),
                V((2, SD, CP), F32),
                V((2, 8, 128), F32),
                V((2, NZ * NC, 8, 128), F32),
                V((2, 8, 128), F32),
                V((2, LINE, 8, 128), F32),
                dma((9,)),
                dma(()),
                dma(()),
                dma(()),
                dma(()),
                dma(()),
                dma((NZ,)),
                dma((2, 2)),
                dma((2, 2, len(RINGS))),
                dma((2, 2)),
                dma((2, 2)),
                dma((2, 2)),
                dma((2, 2)),
                dma((2,)),
                dma((2,)),
                dma((2,)),
                dma((2,)),
            ],
            compiler_params=pltpu.CompilerParams(
                collective_id=0, has_side_effects=True
            ),
        )(
            right_side,
            positions,
            sphere_radii.reshape(1, SD),
            azimuths.reshape(1, SD),
            pair_flags,
            pair_counts.reshape(1, SD),
            tilt_matrix,
            axial_terms,
            jnp.asarray(orders_rows()),
        )
    )
    return tuple(
        pl.pallas_call(
            put_out,
            name="put_out",
            out_shape=(out, out, out),
            in_specs=[vmem] * 3,
            out_specs=(vmem,) * 3,
        )(*results)
    )


def solution(mesh):
    split_mesh = Mesh(mesh.devices.reshape(NX, NY, NZ, NC), SPH)
    placed = (P(SPH, None, None), P(None, SPH), P(SPH), P(SPH), P(SPH, None), P(SPH), P(), P())
    return jax.shard_map(
        on_device,
        mesh=split_mesh,
        in_specs=placed,
        out_specs=(P(SPH, None, None), P(SPH, None, None), P(SPH, None, None)),
        check_vma=False,
    )
```

```python
import functools

import jax
import jax.numpy as jnp
import numpy as np
from jax import lax
from jax.experimental import pallas as pl
from jax.experimental.pallas import tpu as pltpu
from jax.sharding import Mesh
from jax.sharding import PartitionSpec as P

DEG = 12
TERMS = 8
SPH = ("sph_0", "sph_1", "sph_2", "sph_3")
NX, NY, NZ, NC = 4, 4, 8, 2
MESH = pl.DeviceIdType.MESH

coupling = 0.25
wavenum = 2.5
phase_step = 0.9
dist_floor = 0.8

SD = 16
HALF = 168
C = 336
CP = 384
LINE = NX * NY
PACKED = 42
SRC = LINE * NC * SD
TGT = NZ * SD
RINGS = (
    ((2, 2), (1, 2), (3, 2), (2, 1), (2, 3)),
    ((0, 2), (2, 0), (1, 1), (1, 3), (3, 1), (3, 3)),
    ((0, 1), (0, 3), (1, 0), (3, 0)),
)
LINE_ORDER = (4, 3, 5, 2, 6, 1, 7)
PLANE_ORDER = tuple(offset for ring in RINGS for offset in ring)
PILLAR_ORDER = tuple((j, core) for j in LINE_ORDER for core in (1, 0)) + ((0, 1),)
BF = jnp.bfloat16
F32 = jnp.float32


def orders_rows():
    orders = np.concatenate([np.arange(-degree, degree + 1) for degree in range(1, DEG + 1)])
    rows = np.zeros((8, CP), np.float32)
    rows[0, :HALF] = orders
    rows[0, HALF:C] = orders
    rows[1, :HALF] = 1.0
    rows[1, HALF:C] = -1.0
    return rows


def sincos(x):
    q = jnp.floor(x * (2.0 / np.pi) + 0.5)
    r = x - q * 1.5703125
    r = r - q * 4.83751296997070312e-4
    r = r - q * 7.54978995489188216e-8
    r2 = r * r
    s = r + r * r2 * (-1.6666654611e-1 + r2 * (8.3321608736e-3 + r2 * (-1.9515295891e-4)))
    c = 1.0 - 0.5 * r2 + r2 * r2 * (
        4.166664568298827e-2 + r2 * (-1.388731625493765e-3 + r2 * 2.443315711809948e-5)
    )
    quad = q - 4.0 * jnp.floor(q * 0.25)
    odd = (quad == 1.0) | (quad == 3.0)
    sin_sign = jnp.where(quad >= 2.0, -1.0, 1.0)
    cos_sign = jnp.where((quad == 1.0) | (quad == 2.0), -1.0, 1.0)
    return jnp.where(odd, c, s) * sin_sign, jnp.where(odd, s, c) * cos_sign


def split(x):
    high = x.astype(BF)
    return high, (x - high.astype(F32)).astype(BF)


def dot(a, b):
    return lax.dot_general(a, b, (((1,), (0,)), ((), ())), preferred_element_type=F32)


def spots():
    lane = lax.broadcasted_iota(jnp.int32, (8, 128), 1)
    row = lax.broadcasted_iota(jnp.int32, (8, 128), 0)
    return lane, row % 4


def pack(put, x):
    lane, phase = spots()
    for k in range(4):
        at = slice(8 * (k % 2), 8 * (k % 2) + 8)
        put(8 * k, x[at, 128 * (k // 2) : 128 * (k // 2) + 128])
    upper, lower = x[0:8, 256:384], x[8:16, 256:384]
    put(32, jnp.where(lane < 80, upper, pltpu.roll(lower, 80, 1)))
    rest = jnp.zeros((8, 128), F32)
    for p in range(4):
        rest = jnp.where((phase == p) & (lane // 32 == p), pltpu.roll(lower, (32 * p + 80) % 128, 1), rest)
    put(40, jnp.concatenate([jnp.sum(rest[4 * q : 4 * q + 4], axis=0, keepdims=True) for q in range(2)], axis=0))


def unpack(tiles, tail):
    lane, phase = spots()
    both = tiles[4]
    upper = jnp.where(lane < 80, both, 0.0)
    wide = jnp.concatenate([jnp.broadcast_to(tail[q : q + 1], (4, 128)) for q in range(2)], axis=0)
    rest = jnp.zeros((8, 128), F32)
    for p in range(4):
        rest = jnp.where(phase == p, pltpu.roll(wide, (48 - 32 * p) % 128, 1), rest)
    lower = jnp.where(lane < 48, pltpu.roll(both, 48, 1), jnp.where(lane < 80, rest, 0.0))
    return jnp.concatenate(
        [
            jnp.concatenate([tiles[0], tiles[1]], axis=0),
            jnp.concatenate([tiles[2], tiles[3]], axis=0),
            jnp.concatenate([upper, lower], axis=0),
        ],
        axis=1,
    )


def lanes_of(x):
    total = jnp.sum(x, axis=0, keepdims=True)
    return total[:, 0:128] + total[:, 128:256] + total[:, 256:384]


def kernel(
    vec_hbm, pos_hbm, rad_hbm, az_hbm, flags_hbm, counts_hbm, tilt_hbm, axial_hbm, rows_hbm,
    sol_ref, res_ref, dir_ref,
    vec_ref, pos_ref, rad_ref, az_ref, flags_ref, counts_ref, tilt_ref, axial, rows_ref, ax_cat, tilt_in, tilt_out, flag_out, flag_in, mine, geo_src_out, geo_tgt_out,
    geo_src, geo_tgt, w_cat, field, f_cat, g_lhs, g_acc, part, part_out, got, vec, img, img2,
    scal_out, scal_a, scal_mid, scal_b,
    in_sem, geo_src_send, geo_src_recv, geo_tgt_send, geo_tgt_recv, flag_send, flag_recv,
    field_send, field_recv, pair_send, pair_recv, part_send, part_recv,
    sa_send, sa_recv, sb_send, sb_recv,
):
    mx, my, mz, mc = (lax.axis_index(name) for name in SPH)
    plane = mx * NY + my

    def plane_peer(offset, core):
        return (lax.rem(mx + offset[0], NX), lax.rem(my + offset[1], NY), mz, core)

    def line_peer(j):
        return (mx, my, lax.rem(mz + j, NZ), mc)

    def pillar_peer(j, core):
        return (mx, my, lax.rem(mz + j, NZ), mc if core == 0 else 1 - mc)

    partner = (mx, my, mz, 1 - mc)

    def remote(src, dst, send, recv, peer):
        return pltpu.make_async_remote_copy(
            src_ref=src, dst_ref=dst, send_sem=send, recv_sem=recv, device_id=peer,
            device_id_type=MESH,
        )

    with jax.named_scope("loads"):
        pairs = (
            (pos_hbm, pos_ref), (rad_hbm, rad_ref), (az_hbm, az_ref), (counts_hbm, counts_ref),
            (rows_hbm, rows_ref), (flags_hbm, flags_ref), (tilt_hbm, tilt_ref), (vec_hbm, vec_ref),
            (axial_hbm, axial),
        )
        loads = [pltpu.make_async_copy(a, b, in_sem.at[k]) for k, (a, b) in enumerate(pairs)]
        for load in loads:
            load.start()

        barrier = pltpu.get_barrier_semaphore()

        def greet(peer):
            pl.semaphore_signal(barrier, inc=1, device_id=peer, device_id_type=MESH)

        for j, core in PILLAR_ORDER:
            greet(pillar_peer(j, core))
        for offset in PLANE_ORDER:
            for core in range(NC):
                greet(plane_peer(offset, core))

        for load in loads[:6]:
            load.wait()

    with jax.named_scope("geo_prep"):
        mine[...] = jnp.zeros((8, 128), F32)
        mine[0:3, 0:SD] = pos_ref[...]
        mine[3:4, 0:SD] = rad_ref[...]
        mine[4:5, 0:SD] = az_ref[...]
        mine[5:6, 0:SD] = counts_ref[...].astype(F32)
        own = mine[...]
        lane = lax.broadcasted_iota(jnp.int32, (8, 128), 1)
        spread = own
        for shift in (16, 32, 64):
            spread = spread + pltpu.roll(spread, shift, 1)
        geo_src_out[...] = jnp.where(lane // SD == lax.rem(plane, 8), spread, 0.0)
        geo_tgt_out[...] = jnp.where(lane // SD == mz, spread, 0.0)
        geo_src[pl.ds(plane, 1)] = geo_src_out[...][None]
        geo_tgt[pl.ds(0, 1)] = geo_tgt_out[...][None]

    with jax.named_scope("flag_prep"):
        lane = lax.broadcasted_iota(jnp.int32, (SD, 128), 1)
        for upper in range(2):
            for eight in range(2):
                sides = ([], [])
                for k in range(4):
                    at = ((8 * eight + 2 * k) * 2 + upper) * 128
                    first, second = flags_ref[:, at : at + 128], flags_ref[:, at + 256 : at + 384]
                    even = jnp.where(lane % 32 < 16, first, pltpu.roll(second, 16, 1))
                    odd = jnp.where(lane % 32 < 16, pltpu.roll(first, 112, 1), second)
                    sides[0].append(jnp.where(mc == 0, even, odd))
                    sides[1].append(jnp.where(mc == 0, odd, even))
                for side in range(2):
                    for r in range(4):
                        tile = sides[side][r]
                        for k in range(4):
                            if k != r:
                                piece = pltpu.roll(sides[side][k], (32 * (k - r)) % 128, 1)
                                tile = jnp.where(lane // 32 == k, piece, tile)
                        at = 128 * (2 * side + eight)
                        flag_out[4 * upper + r, :, at : at + 128] = tile

    loads[6].wait()
    loads[7].wait()
    cols = jnp.transpose(jnp.concatenate([own] * 16, axis=0))
    azimuth = cols[0:SD, 4:5]
    root = 1.0 / jnp.sqrt(1.0 + cols[0:SD, 5:6])
    sin_az, cos_az = sincos(azimuth * rows_ref[0:1, :])
    sin_az = sin_az * rows_ref[1:2, :]
    zeros_pad = jnp.zeros((CP - C, CP), BF)
    turned = jnp.concatenate([tilt_ref[HALF:C, :], tilt_ref[0:HALF, :]], axis=0)
    for half, block in enumerate((tilt_ref[...], turned)):
        block = jnp.concatenate([block, jnp.zeros((C, CP - C), F32)], axis=1)
        for which, value in enumerate(split(block)):
            at = slice(which * CP, (which + 1) * CP)
            tilt_in[half * CP : half * CP + C, at] = value
            tilt_in[half * CP + C : (half + 1) * CP, at] = zeros_pad

    def halves_sum(r, width):
        return r[0:SD, 0:width] + r[SD : 2 * SD, 0:width] + r[0:SD, width : 2 * width]

    def to_frame(x):
        parts = split(jnp.concatenate([x * cos_az, x * sin_az], axis=1))
        return halves_sum(dot(jnp.concatenate(parts, axis=0), tilt_in[...]), CP)

    def from_frame(x):
        u = halves_sum(dot(jnp.concatenate(split(x), axis=0), tilt_out[...]), 2 * CP)
        return (u[:, 0:CP] * cos_az + u[:, CP : 2 * CP] * sin_az) * root

    def keep(a, h, framed):
        def put(row, value):
            field[a, h, plane, row : row + value.shape[0], :] = value

        pack(put, framed)

    with jax.named_scope("frame0"):
        for h in range(2):
            v = jnp.concatenate([vec_ref[:, h, :], jnp.zeros((SD, CP - C), F32)], axis=1)
            vec[h] = v
            keep(0, h, to_frame(v))

    with jax.named_scope("barrier_wait"):
        pl.semaphore_wait(barrier, 2 * (LINE - 1) + NZ * NC - 1)

    def src_copy(peer, other):
        to = geo_src.at[LINE * other + plane]
        return remote(geo_src_out, to, geo_src_send, geo_src_recv, peer)

    src_all_copies = remote(
        geo_src.at[pl.ds(0, LINE * NC - 1)], geo_src.at[pl.ds(0, LINE * NC - 1)],
        geo_src_send, geo_src_recv, partner,
    )

    def tgt_copy(j):
        return remote(geo_tgt_out, geo_tgt.at[j], geo_tgt_send, geo_tgt_recv, line_peer(j))

    tgt_all_copies = remote(
        geo_tgt.at[pl.ds(0, NZ - 1)], geo_tgt.at[pl.ds(0, NZ - 1)],
        geo_tgt_send, geo_tgt_recv, partner,
    )

    def flag_copy(j):
        to = lax.rem(mz + j, NZ)
        return remote(flag_out.at[to], flag_in.at[j], flag_send, flag_recv.at[j], line_peer(j))

    def blocks(a, h, count, send, recv):
        at = field.at[a, h, pl.ds(0, count), pl.ds(0, PACKED), :]
        return remote(at, at, send, recv, partner)

    def packed_block(a, h, k):
        return field.at[a, h, k, pl.ds(0, PACKED), :]

    def field_copy(a, h, ring, offset):
        at = packed_block(a, h, plane)
        return remote(at, at, field_send.at[a, h], field_recv.at[a, h, ring], plane_peer(offset, mc))

    def pair_copy(a, h, offset):
        source = lax.rem(mx + NX - offset[0], NX) * NY + lax.rem(my + NY - offset[1], NY)
        return remote(
            packed_block(a, h, source), packed_block(a, h, LINE + source), pair_send.at[a, h], pair_recv.at[a, h],
            partner,
        )

    def send_part(a, h):
        for z in range(NZ):

            def put(row, value):
                part_out[a, h, z, row : row + value.shape[0], :] = value

            pack(put, part[z * SD : (z + 1) * SD, :])
        for k, j in enumerate(LINE_ORDER):
            remote(
                part_out.at[a, h, lax.rem(mz + j, NZ), pl.ds(0, PACKED), :],
                got.at[a, h, k, pl.ds(0, PACKED), :],
                part_send.at[a, h], part_recv.at[a, h], line_peer(j),
            ).start()

    def part_all(a, h):
        at = got.at[a, h, pl.ds(0, NZ - 1), pl.ds(0, PACKED), :]
        return remote(at, at, part_send.at[a, h], part_recv.at[a, h], partner)

    def send_pillar(r):
        for k, (j, core) in enumerate(PILLAR_ORDER):
            remote(
                scal_out.at[r], scal_a.at[r, k], sa_send.at[r], sa_recv.at[r], pillar_peer(j, core)
            ).start()

    def sa_all(r):
        at = scal_a.at[r, pl.ds(0, NZ * NC - 1)]
        return remote(at, at, sa_send.at[r], sa_recv.at[r], partner)

    def send_plane(r):
        for k, offset in enumerate(PLANE_ORDER):
            remote(
                scal_mid.at[r], scal_b.at[r, k], sb_send.at[r], sb_recv.at[r],
                plane_peer(offset, mc),
            ).start()

    def sb_all(r):
        at = scal_b.at[r, pl.ds(0, LINE - 1)]
        return remote(at, at, sb_send.at[r], sb_recv.at[r], partner)

    def send_field(a, h):
        for ring, offsets in enumerate(RINGS):
            for offset in offsets:
                field_copy(a, h, ring, offset).start()
        pair_copy(a, h, (0, 0)).start()

    def relay(a, h, ring):
        with jax.named_scope(f"relay{a}{h}{ring}"):
            blocks(a, h, len(RINGS[ring]), field_send.at[a, h], field_recv.at[a, h, ring]).wait_recv()
            for offset in RINGS[ring]:
                pair_copy(a, h, offset).start()

    with jax.named_scope("sends"):
        for offset in PLANE_ORDER:
            for other in range(NC):
                src_copy(plane_peer(offset, 1 - mc if other else mc), other).start()
        src_copy(partner, 1).start()
        for j in LINE_ORDER:
            tgt_copy(j).start()
        for j in LINE_ORDER:
            flag_copy(j).start()
        send_field(0, 0)
        send_field(0, 1)

    with jax.named_scope("axial"):
        loads[8].wait()
        for m in range(TERMS):
            block = jnp.concatenate([axial[m], jnp.zeros((C, CP - C), F32)], axis=1)
            for which, value in enumerate(split(block)):
                at = slice(which * CP, (which + 1) * CP)
                ax_cat[m * CP : m * CP + C, at] = value
                ax_cat[m * CP + C : (m + 1) * CP, at] = zeros_pad
        for which in range(2):
            for half in range(2):
                at = (which * 2 + half) * CP
                tilt_out[:, at : at + CP] = jnp.transpose(
                    tilt_in[half * CP : (half + 1) * CP, which * CP : (which + 1) * CP].astype(F32)
                ).astype(BF)

    with jax.named_scope("geo_wait"):
        src_all_copies.wait_recv()
        tgt_all_copies.wait_recv()
    src_rows = []
    for tile in range(SRC // 128):
        total = geo_src[8 * tile]
        for k in range(1, 8):
            total = total + geo_src[8 * tile + k]
        src_rows.append(total)
    src_all = jnp.concatenate(src_rows, axis=1)
    tgt_all = geo_tgt[0]
    for j in range(1, NZ):
        tgt_all = tgt_all + geo_tgt[j]
    part[:, 0:128] = jnp.transpose(jnp.concatenate([tgt_all] * 16, axis=0))

    def weigh(flags, z):
        rows = pl.ds(pl.multiple_of(z * SD, SD), SD)
        tgt = part[rows, 0:128]
        dx = tgt[:, 0:1] - src_all[0:1, :]
        dy = tgt[:, 1:2] - src_all[1:2, :]
        dz = tgt[:, 2:3] - src_all[2:3, :]
        dist = jnp.sqrt(dx * dx + dy * dy + dz * dz)
        ratio = (tgt[:, 3:4] + src_all[3:4, :]) / jnp.maximum(dist, dist_floor)
        sin_d, cos_d = sincos(wavenum * dist)
        scale = jnp.where(flags != 0, coupling, 0.0)
        near = jnp.where(flags == 1, coupling, 0.0)
        for m in range(TERMS):
            if m > 0:
                near = near * ratio
                scale = near
            wave = cos_d * float(np.cos(phase_step * m)) - sin_d * float(np.sin(phase_step * m))
            high, low = split(wave * scale)
            at = pl.ds(pl.multiple_of(m * TGT + z * SD, SD), SD)
            for side in range(2):
                for k, value in enumerate((high, high, low)):
                    to = (3 * side + k) * 256
                    w_cat[at, to : to + 256] = value[:, side * 256 : (side + 1) * 256]

    with jax.named_scope("weigh"):
        weigh(flag_out[mz], mz)

        def weigh_from(j, carry):
            flag_copy(j).wait_recv()
            weigh(flag_in[j], lax.rem(mz + NZ - j, NZ))
            return carry

        for ring, (lo, hi) in enumerate(((1, 3), (3, 6), (6, 8))):
            relay(0, 0, ring)
            lax.fori_loop(lo, hi, weigh_from, 0)

    def reduce_pillar(r):
        with jax.named_scope(f"pillar_wait{r}"):
            sa_all(r).wait_recv()
        total = scal_out[r]
        for k in range(NZ * NC - 1):
            total = total + scal_a[r, k]
        scal_mid[r] = total
        send_plane(r)

    def reduce_plane(r):
        with jax.named_scope(f"plane_wait{r}"):
            sb_all(r).wait_recv()
        total = scal_mid[r]
        for k in range(LINE - 1):
            total = total + scal_b[r, k]
        return jnp.sum(total, axis=1, keepdims=True)

    def couple(a, h):
        def unfold(side):
            for k in range(LINE):
                tiles = [field[a, h, LINE * side + k, 8 * t : 8 * t + 8, :] for t in range(5)]
                tail = field[a, h, LINE * side + k, 40:42, :]
                high, low = split(unpack(tiles, tail))
                for t, value in enumerate((high, low, high)):
                    row = (3 * side + t) * 256 + k * SD
                    f_cat[row : row + SD, :] = value

        def arrive():
            with jax.named_scope(f"gather_wait{a}{h}"):
                blocks(a, h, LINE, pair_send.at[a, h], pair_recv.at[a, h]).wait_recv()

        if h == 1:
            arrive()
        with jax.named_scope(f"early{a}{h}"):
            unfold(0)
            if h == 0:
                for piece in range(2):
                    at = slice(piece * 512, (piece + 1) * 512)
                    g_acc[at, :] = dot(w_cat[at, 0:768], f_cat[0:768, :])
        if h == 0:
            arrive()
        with jax.named_scope(f"first{a}{h}"):
            unfold(1)
            for piece in range(2):
                at = slice(piece * 512, (piece + 1) * 512)
                if h == 0:
                    g = g_acc[at, :] + dot(w_cat[at, 768:1536], f_cat[768:1536, :])
                else:
                    g = dot(w_cat[at, :], f_cat[...])
                g_high, g_low = split(g)
                for k in range(4):
                    m = piece * 4 + k
                    g_lhs[0:TGT, m * CP : (m + 1) * CP] = g_high[k * TGT : (k + 1) * TGT]
                    g_lhs[TGT : 2 * TGT, m * CP : (m + 1) * CP] = g_low[k * TGT : (k + 1) * TGT]
        if h == 0:
            for ring in range(len(RINGS)):
                relay(a, 1, ring)
            if a == 1:
                reduce_pillar(0)
        with jax.named_scope(f"second{a}{h}"):
            both = dot(g_lhs[...], ax_cat[:, 0:CP])
            part[...] = both[0:TGT] + both[TGT : 2 * TGT] + dot(g_lhs[0:TGT, :], ax_cat[:, CP : 2 * CP])
            send_part(a, h)

    def collect(a, h):
        with jax.named_scope(f"part_wait{a}{h}"):
            part_all(a, h).wait_recv()

        def summed(lo, hi):
            total = part_out[a, h, mz, lo:hi, :]
            for k in range(NZ - 1):
                total = total + got[a, h, k, lo:hi, :]
            return total

        total = unpack([summed(8 * t, 8 * t + 8) for t in range(5)], summed(40, 42))
        return from_frame(total)

    couple(0, 0)
    couple(0, 1)
    for h in range(2):
        image = vec[h] - collect(0, h)
        img[h] = image
        keep(1, h, to_frame(image))
        send_field(1, h)

    scal_out[...] = jnp.zeros((2, 8, 128), F32)
    scal_out[0, 0:1, :] = lanes_of(vec[0] * vec[0] + vec[1] * vec[1])
    scal_out[0, 1:2, :] = lanes_of(vec[0] * img[0] + vec[1] * img[1])
    send_pillar(0)
    for ring in range(len(RINGS)):
        relay(1, 0, ring)
    couple(1, 0)
    couple(1, 1)
    seconds = [img[h] - collect(1, h) for h in range(2)]
    sums = reduce_plane(0)
    rho_start = sums[0:1, :]
    alpha = rho_start / sums[1:2, :]

    def inner(left, right):
        return lanes_of(left[0] * right[0] + left[1] * right[1])

    half_step = []
    half_image = []
    for h in range(2):
        image = img[h]
        half_step.append(vec[h] - alpha * image)
        half_image.append(image - alpha * seconds[h])
    right = [vec[0], vec[1]]
    scal_out[1, 0:1, :] = inner(half_image, half_step)
    scal_out[1, 1:2, :] = inner(half_image, half_image)
    scal_out[1, 2:3, :] = inner(right, half_step)
    scal_out[1, 3:4, :] = inner(right, half_image)
    send_pillar(1)
    reduce_pillar(1)
    sums = reduce_plane(1)
    omega = sums[0:1, :] / sums[1:2, :]
    rho_next = sums[2:3, :] - omega * sums[3:4, :]
    beta = rho_next / rho_start * (alpha / omega)
    for h in range(2):
        res = half_step[h] - omega * half_image[h]
        sol_ref[:, h, :] = (alpha * right[h] + omega * half_step[h])[:, 0:C]
        res_ref[:, h, :] = res[:, 0:C]
        dir_ref[:, h, :] = (res + beta * (right[h] - omega * img[h]))[:, 0:C]

    with jax.named_scope("drain"):
        src_all_copies.wait_send()
        tgt_all_copies.wait_send()
        sent = flag_in.at[pl.ds(0, NZ - 1)]
        remote(sent, sent, flag_send, flag_recv.at[0], partner).wait_send()
        for a in range(2):
            for h in range(2):
                blocks(a, h, LINE - 1, field_send.at[a, h], field_recv.at[a, h, 0]).wait_send()
                blocks(a, h, LINE, pair_send.at[a, h], pair_recv.at[a, h]).wait_send()
                part_all(a, h).wait_send()
            sa_all(a).wait_send()
            sb_all(a).wait_send()


def put_out(*refs):
    ins, outs, sems = refs[:3], refs[3:6], refs[6]
    copies = [pltpu.make_async_copy(a, b, sems.at[k]) for k, (a, b) in enumerate(zip(ins, outs))]
    for copy in copies:
        copy.start()
    for copy in copies:
        copy.wait()


def on_device(
    right_side, positions, sphere_radii, azimuths, pair_flags, pair_counts, tilt_matrix, axial_terms
):
    vmem = pl.BlockSpec(memory_space=pltpu.VMEM)
    hbm = pl.BlockSpec(memory_space=pltpu.HBM)
    dma = pltpu.SemaphoreType.DMA
    out = jax.ShapeDtypeStruct((SD, 2, C), F32)
    V = pltpu.VMEM
    results = tuple(
        pl.pallas_call(
            kernel,
            name="bicgstab",
            out_shape=(out, out, out),
            in_specs=[hbm] * 9,
            out_specs=(vmem, vmem, vmem),
            scratch_shapes=[
                V((SD, 2, C), F32),
                V((3, SD), F32),
                V((1, SD), F32),
                V((1, SD), F32),
                V((SD, LINE * NZ * NC * SD), jnp.int32),
                V((1, SD), jnp.int32),
                V((C, C), F32),
                V((TERMS, C, C), F32),
                V((8, CP), F32),
                V((TERMS * CP, 2 * CP), BF),
                V((2 * CP, 2 * CP), BF),
                V((CP, 4 * CP), BF),
                V((NZ, SD, SRC), jnp.int32),
                V((NZ, SD, SRC), jnp.int32),
                V((8, 128), F32),
                V((8, 128), F32),
                V((8, 128), F32),
                V((LINE * NC, 8, 128), F32),
                V((NZ, 8, 128), F32),
                V((TERMS * TGT, 3 * SRC), BF),
                V((2, 2, LINE * NC, 48, 128), F32),
                V((3 * SRC, CP), BF),
                V((2 * TGT, TERMS * CP), BF),
                V((TERMS * TGT, CP), F32),
                V((TGT, CP), F32),
                V((2, 2, NZ, 48, 128), F32),
                V((2, 2, NZ, 48, 128), F32),
                V((2, SD, CP), F32),
                V((2, SD, CP), F32),
                V((2, SD, CP), F32),
                V((2, 8, 128), F32),
                V((2, NZ * NC, 8, 128), F32),
                V((2, 8, 128), F32),
                V((2, LINE, 8, 128), F32),
                dma((9,)),
                dma(()),
                dma(()),
                dma(()),
                dma(()),
                dma(()),
                dma((NZ,)),
                dma((2, 2)),
                dma((2, 2, len(RINGS))),
                dma((2, 2)),
                dma((2, 2)),
                dma((2, 2)),
                dma((2, 2)),
                dma((2,)),
                dma((2,)),
                dma((2,)),
                dma((2,)),
            ],
            compiler_params=pltpu.CompilerParams(
                collective_id=0, has_side_effects=True, vmem_limit_bytes=48 * 1024 * 1024
            ),
        )(
            *(
                pltpu.with_memory_space_constraint(x, pltpu.HBM)
                for x in (
                    right_side,
                    positions,
                    sphere_radii.reshape(1, SD),
                    azimuths.reshape(1, SD),
                    pair_flags,
                    pair_counts.reshape(1, SD),
                    tilt_matrix,
                    axial_terms,
                    jnp.asarray(orders_rows()),
                )
            )
        )
    )
    return tuple(
        pl.pallas_call(
            put_out,
            name="put_out",
            out_shape=(out, out, out),
            in_specs=[vmem] * 3,
            out_specs=(hbm,) * 3,
            scratch_shapes=[dma((3,))],
            compiler_params=pltpu.CompilerParams(vmem_limit_bytes=2 * 1024 * 1024),
        )(*results)
    )


def solution(mesh):
    split_mesh = Mesh(mesh.devices.reshape(NX, NY, NZ, NC), SPH)
    placed = (P(SPH, None, None), P(None, SPH), P(SPH), P(SPH), P(SPH, None), P(SPH), P(), P())
    return jax.shard_map(
        on_device,
        mesh=split_mesh,
        in_specs=placed,
        out_specs=(P(SPH, None, None), P(SPH, None, None), P(SPH, None, None)),
        check_vma=False,
    )
```

```python
import functools

import jax
import jax.numpy as jnp
import numpy as np
from jax import lax
from jax.experimental import pallas as pl
from jax.experimental.pallas import tpu as pltpu
from jax.sharding import Mesh
from jax.sharding import PartitionSpec as P

DEG = 12
TERMS = 8
SPH = ("sph_0", "sph_1", "sph_2", "sph_3")
NX, NY, NZ, NC = 4, 4, 8, 2
MESH = pl.DeviceIdType.MESH

coupling = 0.25
wavenum = 2.5
phase_step = 0.9
dist_floor = 0.8

SD = 16
HALF = 168
C = 336
CP = 384
LINE = NX * NY
PACKED = 42
SRC = LINE * NC * SD
TGT = NZ * SD
RINGS = (
    ((2, 2), (1, 2), (3, 2), (2, 1), (2, 3)),
    ((0, 2), (2, 0), (1, 1), (1, 3), (3, 1), (3, 3)),
    ((0, 1), (0, 3), (1, 0), (3, 0)),
)
LINE_ORDER = (4, 3, 5, 2, 6, 1, 7)
PLANE_ORDER = tuple(offset for ring in RINGS for offset in ring)
PILLAR_ORDER = tuple((j, core) for j in LINE_ORDER for core in (1, 0)) + ((0, 1),)
BF = jnp.bfloat16
F32 = jnp.float32


def orders_rows():
    orders = np.concatenate([np.arange(-degree, degree + 1) for degree in range(1, DEG + 1)])
    rows = np.zeros((8, CP), np.float32)
    rows[0, :HALF] = orders
    rows[0, HALF:C] = orders
    rows[1, :HALF] = 1.0
    rows[1, HALF:C] = -1.0
    return rows


def sincos(x):
    q = jnp.floor(x * (2.0 / np.pi) + 0.5)
    r = x - q * 1.5703125
    r = r - q * 4.83751296997070312e-4
    r = r - q * 7.54978995489188216e-8
    r2 = r * r
    s = r + r * r2 * (-1.6666654611e-1 + r2 * (8.3321608736e-3 + r2 * (-1.9515295891e-4)))
    c = 1.0 - 0.5 * r2 + r2 * r2 * (
        4.166664568298827e-2 + r2 * (-1.388731625493765e-3 + r2 * 2.443315711809948e-5)
    )
    quad = q - 4.0 * jnp.floor(q * 0.25)
    odd = (quad == 1.0) | (quad == 3.0)
    sin_sign = jnp.where(quad >= 2.0, -1.0, 1.0)
    cos_sign = jnp.where((quad == 1.0) | (quad == 2.0), -1.0, 1.0)
    return jnp.where(odd, c, s) * sin_sign, jnp.where(odd, s, c) * cos_sign


def split(x):
    high = x.astype(BF)
    return high, (x - high.astype(F32)).astype(BF)


def dot(a, b):
    return lax.dot_general(a, b, (((1,), (0,)), ((), ())), preferred_element_type=F32)


def spots():
    lane = lax.broadcasted_iota(jnp.int32, (8, 128), 1)
    row = lax.broadcasted_iota(jnp.int32, (8, 128), 0)
    return lane, row % 4


def pack(put, x):
    lane, phase = spots()
    for k in range(4):
        at = slice(8 * (k % 2), 8 * (k % 2) + 8)
        put(8 * k, x[at, 128 * (k // 2) : 128 * (k // 2) + 128])
    upper, lower = x[0:8, 256:384], x[8:16, 256:384]
    put(32, jnp.where(lane < 80, upper, pltpu.roll(lower, 80, 1)))
    rest = jnp.zeros((8, 128), F32)
    for p in range(4):
        rest = jnp.where((phase == p) & (lane // 32 == p), pltpu.roll(lower, (32 * p + 80) % 128, 1), rest)
    put(40, jnp.concatenate([jnp.sum(rest[4 * q : 4 * q + 4], axis=0, keepdims=True) for q in range(2)], axis=0))


def unpack(tiles, tail):
    lane, phase = spots()
    both = tiles[4]
    upper = jnp.where(lane < 80, both, 0.0)
    wide = jnp.concatenate([jnp.broadcast_to(tail[q : q + 1], (4, 128)) for q in range(2)], axis=0)
    rest = jnp.zeros((8, 128), F32)
    for p in range(4):
        rest = jnp.where(phase == p, pltpu.roll(wide, (48 - 32 * p) % 128, 1), rest)
    lower = jnp.where(lane < 48, pltpu.roll(both, 48, 1), jnp.where(lane < 80, rest, 0.0))
    return jnp.concatenate(
        [
            jnp.concatenate([tiles[0], tiles[1]], axis=0),
            jnp.concatenate([tiles[2], tiles[3]], axis=0),
            jnp.concatenate([upper, lower], axis=0),
        ],
        axis=1,
    )


def lanes_of(x):
    total = jnp.sum(x, axis=0, keepdims=True)
    return total[:, 0:128] + total[:, 128:256] + total[:, 256:384]


def kernel(
    vec_hbm, pos_hbm, rad_hbm, az_hbm, flags_hbm, counts_hbm, tilt_hbm, axial_hbm, rows_hbm,
    sol_ref, res_ref, dir_ref,
    vec_ref, pos_ref, rad_ref, az_ref, flags_ref, counts_ref, tilt_ref, axial, rows_ref, ax_cat, tilt_in, tilt_out, flag_out, flag_in, mine, geo_src_out, geo_tgt_out,
    geo_src, geo_tgt, w_cat, field, f_cat, g_lhs, g_acc, part, part_out, got, vec, img, img2,
    scal_out, scal_a, scal_mid, scal_b,
    in_sem, geo_src_send, geo_src_recv, geo_tgt_send, geo_tgt_recv, flag_send, flag_recv,
    field_send, field_recv, pair_send, pair_recv, part_send, part_recv,
    sa_send, sa_recv, sb_send, sb_recv,
):
    mx, my, mz, mc = (lax.axis_index(name) for name in SPH)
    plane = mx * NY + my

    def plane_peer(offset, core):
        return (lax.rem(mx + offset[0], NX), lax.rem(my + offset[1], NY), mz, core)

    def line_peer(j):
        return (mx, my, lax.rem(mz + j, NZ), mc)

    def pillar_peer(j, core):
        return (mx, my, lax.rem(mz + j, NZ), mc if core == 0 else 1 - mc)

    partner = (mx, my, mz, 1 - mc)

    def remote(src, dst, send, recv, peer):
        return pltpu.make_async_remote_copy(
            src_ref=src, dst_ref=dst, send_sem=send, recv_sem=recv, device_id=peer,
            device_id_type=MESH,
        )

    with jax.named_scope("loads"):
        pairs = (
            (pos_hbm, pos_ref), (rad_hbm, rad_ref), (az_hbm, az_ref), (counts_hbm, counts_ref),
            (rows_hbm, rows_ref), (flags_hbm, flags_ref), (tilt_hbm, tilt_ref), (vec_hbm, vec_ref),
            (axial_hbm, axial),
        )
        loads = [pltpu.make_async_copy(a, b, in_sem.at[k]) for k, (a, b) in enumerate(pairs)]
        for load in loads:
            load.start()

        barrier = pltpu.get_barrier_semaphore()

        def greet(peer):
            pl.semaphore_signal(barrier, inc=1, device_id=peer, device_id_type=MESH)

        for j, core in PILLAR_ORDER:
            greet(pillar_peer(j, core))
        for offset in PLANE_ORDER:
            for core in range(NC):
                greet(plane_peer(offset, core))

        for load in loads[:6]:
            load.wait()

    with jax.named_scope("geo_prep"):
        mine[...] = jnp.zeros((8, 128), F32)
        mine[0:3, 0:SD] = pos_ref[...]
        mine[3:4, 0:SD] = rad_ref[...]
        mine[4:5, 0:SD] = az_ref[...]
        mine[5:6, 0:SD] = counts_ref[...].astype(F32)
        own = mine[...]
        lane = lax.broadcasted_iota(jnp.int32, (8, 128), 1)
        spread = own
        for shift in (16, 32, 64):
            spread = spread + pltpu.roll(spread, shift, 1)
        geo_src_out[...] = jnp.where(lane // SD == lax.rem(plane, 8), spread, 0.0)
        geo_tgt_out[...] = jnp.where(lane // SD == mz, spread, 0.0)
        geo_src[pl.ds(plane, 1)] = geo_src_out[...][None]
        geo_tgt[pl.ds(0, 1)] = geo_tgt_out[...][None]

    with jax.named_scope("flag_prep"):
        lane = lax.broadcasted_iota(jnp.int32, (SD, 128), 1)
        for upper in range(2):
            for eight in range(2):
                sides = ([], [])
                for k in range(4):
                    at = ((8 * eight + 2 * k) * 2 + upper) * 128
                    first, second = flags_ref[:, at : at + 128], flags_ref[:, at + 256 : at + 384]
                    even = jnp.where(lane % 32 < 16, first, pltpu.roll(second, 16, 1))
                    odd = jnp.where(lane % 32 < 16, pltpu.roll(first, 112, 1), second)
                    sides[0].append(jnp.where(mc == 0, even, odd))
                    sides[1].append(jnp.where(mc == 0, odd, even))
                for side in range(2):
                    for r in range(4):
                        tile = sides[side][r]
                        for k in range(4):
                            if k != r:
                                piece = pltpu.roll(sides[side][k], (32 * (k - r)) % 128, 1)
                                tile = jnp.where(lane // 32 == k, piece, tile)
                        at = 128 * (2 * side + eight)
                        flag_out[4 * upper + r, :, at : at + 128] = tile

    with jax.named_scope("barrier_wait"):
        pl.semaphore_wait(barrier, 2 * (LINE - 1) + NZ * NC - 1)

    def src_copy(peer, other):
        to = geo_src.at[LINE * other + plane]
        return remote(geo_src_out, to, geo_src_send, geo_src_recv, peer)

    src_all_copies = remote(
        geo_src.at[pl.ds(0, LINE * NC - 1)], geo_src.at[pl.ds(0, LINE * NC - 1)],
        geo_src_send, geo_src_recv, partner,
    )

    def tgt_copy(j):
        return remote(geo_tgt_out, geo_tgt.at[j], geo_tgt_send, geo_tgt_recv, line_peer(j))

    tgt_all_copies = remote(
        geo_tgt.at[pl.ds(0, NZ - 1)], geo_tgt.at[pl.ds(0, NZ - 1)],
        geo_tgt_send, geo_tgt_recv, partner,
    )

    def flag_copy(j):
        to = lax.rem(mz + j, NZ)
        return remote(flag_out.at[to], flag_in.at[j], flag_send, flag_recv.at[j], line_peer(j))

    def blocks(a, h, count, send, recv):
        at = field.at[a, h, pl.ds(0, count), pl.ds(0, PACKED), :]
        return remote(at, at, send, recv, partner)

    def packed_block(a, h, k):
        return field.at[a, h, k, pl.ds(0, PACKED), :]

    def field_copy(a, h, ring, offset):
        at = packed_block(a, h, plane)
        return remote(at, at, field_send.at[a, h], field_recv.at[a, h, ring], plane_peer(offset, mc))

    def pair_copy(a, h, offset):
        source = lax.rem(mx + NX - offset[0], NX) * NY + lax.rem(my + NY - offset[1], NY)
        return remote(
            packed_block(a, h, source), packed_block(a, h, LINE + source), pair_send.at[a, h], pair_recv.at[a, h],
            partner,
        )

    def send_part(a, h):
        for z in range(NZ):

            def put(row, value):
                part_out[a, h, z, row : row + value.shape[0], :] = value

            pack(put, part[z * SD : (z + 1) * SD, :])
        for k, j in enumerate(LINE_ORDER):
            remote(
                part_out.at[a, h, lax.rem(mz + j, NZ), pl.ds(0, PACKED), :],
                got.at[a, h, k, pl.ds(0, PACKED), :],
                part_send.at[a, h], part_recv.at[a, h], line_peer(j),
            ).start()

    def part_all(a, h):
        at = got.at[a, h, pl.ds(0, NZ - 1), pl.ds(0, PACKED), :]
        return remote(at, at, part_send.at[a, h], part_recv.at[a, h], partner)

    def send_pillar(r):
        for k, (j, core) in enumerate(PILLAR_ORDER):
            remote(
                scal_out.at[r], scal_a.at[r, k], sa_send.at[r], sa_recv.at[r], pillar_peer(j, core)
            ).start()

    def sa_all(r):
        at = scal_a.at[r, pl.ds(0, NZ * NC - 1)]
        return remote(at, at, sa_send.at[r], sa_recv.at[r], partner)

    def send_plane(r):
        for k, offset in enumerate(PLANE_ORDER):
            remote(
                scal_mid.at[r], scal_b.at[r, k], sb_send.at[r], sb_recv.at[r],
                plane_peer(offset, mc),
            ).start()

    def sb_all(r):
        at = scal_b.at[r, pl.ds(0, LINE - 1)]
        return remote(at, at, sb_send.at[r], sb_recv.at[r], partner)

    def send_field(a, h):
        for ring, offsets in enumerate(RINGS):
            for offset in offsets:
                field_copy(a, h, ring, offset).start()
        pair_copy(a, h, (0, 0)).start()

    def relay(a, h, ring):
        with jax.named_scope(f"relay{a}{h}{ring}"):
            blocks(a, h, len(RINGS[ring]), field_send.at[a, h], field_recv.at[a, h, ring]).wait_recv()
            for offset in RINGS[ring]:
                pair_copy(a, h, offset).start()

    with jax.named_scope("sends"):
        for j in LINE_ORDER:
            tgt_copy(j).start()
        for offset in PLANE_ORDER:
            for other in range(NC):
                src_copy(plane_peer(offset, 1 - mc if other else mc), other).start()
        src_copy(partner, 1).start()
        for j in LINE_ORDER:
            flag_copy(j).start()

    loads[6].wait()
    loads[7].wait()
    cols = jnp.transpose(jnp.concatenate([own] * 16, axis=0))
    azimuth = cols[0:SD, 4:5]
    root = 1.0 / jnp.sqrt(1.0 + cols[0:SD, 5:6])
    sin_az, cos_az = sincos(azimuth * rows_ref[0:1, :])
    sin_az = sin_az * rows_ref[1:2, :]
    zeros_pad = jnp.zeros((CP - C, CP), BF)
    turned = jnp.concatenate([tilt_ref[HALF:C, :], tilt_ref[0:HALF, :]], axis=0)
    for half, block in enumerate((tilt_ref[...], turned)):
        block = jnp.concatenate([block, jnp.zeros((C, CP - C), F32)], axis=1)
        for which, value in enumerate(split(block)):
            at = slice(which * CP, (which + 1) * CP)
            tilt_in[half * CP : half * CP + C, at] = value
            tilt_in[half * CP + C : (half + 1) * CP, at] = zeros_pad

    def halves_sum(r, width):
        return r[0:SD, 0:width] + r[SD : 2 * SD, 0:width] + r[0:SD, width : 2 * width]

    def to_frame(x):
        parts = split(jnp.concatenate([x * cos_az, x * sin_az], axis=1))
        return halves_sum(dot(jnp.concatenate(parts, axis=0), tilt_in[...]), CP)

    def from_frame(x):
        u = halves_sum(dot(jnp.concatenate(split(x), axis=0), tilt_out[...]), 2 * CP)
        return (u[:, 0:CP] * cos_az + u[:, CP : 2 * CP] * sin_az) * root

    def keep(a, h, framed):
        def put(row, value):
            field[a, h, plane, row : row + value.shape[0], :] = value

        pack(put, framed)

    with jax.named_scope("frame0"):
        for h in range(2):
            v = jnp.concatenate([vec_ref[:, h, :], jnp.zeros((SD, CP - C), F32)], axis=1)
            vec[h] = v
            keep(0, h, to_frame(v))

    with jax.named_scope("send_fields"):
        send_field(0, 0)
        send_field(0, 1)

    with jax.named_scope("axial"):
        loads[8].wait()
        for m in range(TERMS):
            block = jnp.concatenate([axial[m], jnp.zeros((C, CP - C), F32)], axis=1)
            for which, value in enumerate(split(block)):
                at = slice(which * CP, (which + 1) * CP)
                ax_cat[m * CP : m * CP + C, at] = value
                ax_cat[m * CP + C : (m + 1) * CP, at] = zeros_pad
        for which in range(2):
            for half in range(2):
                at = (which * 2 + half) * CP
                tilt_out[:, at : at + CP] = jnp.transpose(
                    tilt_in[half * CP : (half + 1) * CP, which * CP : (which + 1) * CP].astype(F32)
                ).astype(BF)

    with jax.named_scope("geo_wait"):
        src_all_copies.wait_recv()
        tgt_all_copies.wait_recv()
    src_rows = []
    for tile in range(SRC // 128):
        total = geo_src[8 * tile]
        for k in range(1, 8):
            total = total + geo_src[8 * tile + k]
        src_rows.append(total)
    src_all = jnp.concatenate(src_rows, axis=1)
    tgt_all = geo_tgt[0]
    for j in range(1, NZ):
        tgt_all = tgt_all + geo_tgt[j]
    part[:, 0:128] = jnp.transpose(jnp.concatenate([tgt_all] * 16, axis=0))

    def weigh(flags, z):
        rows = pl.ds(pl.multiple_of(z * SD, SD), SD)
        tgt = part[rows, 0:128]
        dx = tgt[:, 0:1] - src_all[0:1, :]
        dy = tgt[:, 1:2] - src_all[1:2, :]
        dz = tgt[:, 2:3] - src_all[2:3, :]
        dist = jnp.sqrt(dx * dx + dy * dy + dz * dz)
        ratio = (tgt[:, 3:4] + src_all[3:4, :]) / jnp.maximum(dist, dist_floor)
        sin_d, cos_d = sincos(wavenum * dist)
        scale = jnp.where(flags != 0, coupling, 0.0)
        near = jnp.where(flags == 1, coupling, 0.0)
        for m in range(TERMS):
            if m > 0:
                near = near * ratio
                scale = near
            wave = cos_d * float(np.cos(phase_step * m)) - sin_d * float(np.sin(phase_step * m))
            high, low = split(wave * scale)
            at = pl.ds(pl.multiple_of(m * TGT + z * SD, SD), SD)
            for side in range(2):
                for k, value in enumerate((high, high, low)):
                    to = (3 * side + k) * 256
                    w_cat[at, to : to + 256] = value[:, side * 256 : (side + 1) * 256]

    with jax.named_scope("weigh"):
        weigh(flag_out[mz], mz)

        def weigh_from(k, carry):
            j = 4 + (k // 2) * (2 * lax.rem(k, 2) - 1)
            flag_copy(j).wait_recv()
            weigh(flag_in[j], lax.rem(mz + NZ - j, NZ))
            return carry

        for ring, (lo, hi) in enumerate(((1, 3), (3, 6), (6, 8))):
            relay(0, 0, ring)
            lax.fori_loop(lo, hi, weigh_from, 0)

    def reduce_pillar(r):
        with jax.named_scope(f"pillar_wait{r}"):
            sa_all(r).wait_recv()
        total = scal_out[r]
        for k in range(NZ * NC - 1):
            total = total + scal_a[r, k]
        scal_mid[r] = total
        send_plane(r)

    def reduce_plane(r):
        with jax.named_scope(f"plane_wait{r}"):
            sb_all(r).wait_recv()
        total = scal_mid[r]
        for k in range(LINE - 1):
            total = total + scal_b[r, k]
        return jnp.sum(total, axis=1, keepdims=True)

    def couple(a, h):
        def unfold(side):
            for k in range(LINE):
                tiles = [field[a, h, LINE * side + k, 8 * t : 8 * t + 8, :] for t in range(5)]
                tail = field[a, h, LINE * side + k, 40:42, :]
                high, low = split(unpack(tiles, tail))
                for t, value in enumerate((high, low, high)):
                    row = (3 * side + t) * 256 + k * SD
                    f_cat[row : row + SD, :] = value

        def arrive():
            with jax.named_scope(f"gather_wait{a}{h}"):
                blocks(a, h, LINE, pair_send.at[a, h], pair_recv.at[a, h]).wait_recv()

        split_phases = h == 0 or a == 1
        if not split_phases:
            arrive()
        with jax.named_scope(f"early{a}{h}"):
            unfold(0)
            if split_phases:
                for piece in range(2):
                    at = slice(piece * 512, (piece + 1) * 512)
                    g_acc[at, :] = dot(w_cat[at, 0:768], f_cat[0:768, :])
        if split_phases:
            arrive()
        with jax.named_scope(f"first{a}{h}"):
            unfold(1)
            for piece in range(2):
                at = slice(piece * 512, (piece + 1) * 512)
                if split_phases:
                    g = g_acc[at, :] + dot(w_cat[at, 768:1536], f_cat[768:1536, :])
                else:
                    g = dot(w_cat[at, :], f_cat[...])
                g_high, g_low = split(g)
                for k in range(4):
                    m = piece * 4 + k
                    g_lhs[0:TGT, m * CP : (m + 1) * CP] = g_high[k * TGT : (k + 1) * TGT]
                    g_lhs[TGT : 2 * TGT, m * CP : (m + 1) * CP] = g_low[k * TGT : (k + 1) * TGT]
        if h == 0 and a == 0:
            for ring in range(len(RINGS)):
                relay(0, 1, ring)
        with jax.named_scope(f"second{a}{h}"):
            both = dot(g_lhs[...], ax_cat[:, 0:CP])
            part[...] = both[0:TGT] + both[TGT : 2 * TGT] + dot(g_lhs[0:TGT, :], ax_cat[:, CP : 2 * CP])
            send_part(a, h)
        if h == 0 and a == 1:
            for ring in range(len(RINGS)):
                relay(1, 1, ring)
            reduce_pillar(0)

    def collect(a, h):
        with jax.named_scope(f"part_wait{a}{h}"):
            part_all(a, h).wait_recv()

        def summed(lo, hi):
            total = part_out[a, h, mz, lo:hi, :]
            for k in range(NZ - 1):
                total = total + got[a, h, k, lo:hi, :]
            return total

        total = unpack([summed(8 * t, 8 * t + 8) for t in range(5)], summed(40, 42))
        return from_frame(total)

    couple(0, 0)
    couple(0, 1)
    for h in range(2):
        image = vec[h] - collect(0, h)
        img[h] = image
        keep(1, h, to_frame(image))
        send_field(1, h)

    scal_out[...] = jnp.zeros((2, 8, 128), F32)
    scal_out[0, 0:1, :] = lanes_of(vec[0] * vec[0] + vec[1] * vec[1])
    scal_out[0, 1:2, :] = lanes_of(vec[0] * img[0] + vec[1] * img[1])
    send_pillar(0)
    for ring in range(len(RINGS)):
        relay(1, 0, ring)
    couple(1, 0)
    couple(1, 1)
    seconds = [img[h] - collect(1, h) for h in range(2)]
    sums = reduce_plane(0)
    rho_start = sums[0:1, :]
    alpha = rho_start / sums[1:2, :]

    def inner(left, right):
        return lanes_of(left[0] * right[0] + left[1] * right[1])

    half_step = []
    half_image = []
    for h in range(2):
        image = img[h]
        half_step.append(vec[h] - alpha * image)
        half_image.append(image - alpha * seconds[h])
    right = [vec[0], vec[1]]
    scal_out[1, 0:1, :] = inner(half_image, half_step)
    scal_out[1, 1:2, :] = inner(half_image, half_image)
    scal_out[1, 2:3, :] = inner(right, half_step)
    scal_out[1, 3:4, :] = inner(right, half_image)
    send_pillar(1)
    reduce_pillar(1)
    sums = reduce_plane(1)
    omega = sums[0:1, :] / sums[1:2, :]
    rho_next = sums[2:3, :] - omega * sums[3:4, :]
    beta = rho_next / rho_start * (alpha / omega)
    for h in range(2):
        res = half_step[h] - omega * half_image[h]
        sol_ref[:, h, :] = (alpha * right[h] + omega * half_step[h])[:, 0:C]
        res_ref[:, h, :] = res[:, 0:C]
        dir_ref[:, h, :] = (res + beta * (right[h] - omega * img[h]))[:, 0:C]

    with jax.named_scope("drain"):
        src_all_copies.wait_send()
        tgt_all_copies.wait_send()
        sent = flag_in.at[pl.ds(0, NZ - 1)]
        remote(sent, sent, flag_send, flag_recv.at[0], partner).wait_send()
        for a in range(2):
            for h in range(2):
                blocks(a, h, LINE - 1, field_send.at[a, h], field_recv.at[a, h, 0]).wait_send()
                blocks(a, h, LINE, pair_send.at[a, h], pair_recv.at[a, h]).wait_send()
                part_all(a, h).wait_send()
            sa_all(a).wait_send()
            sb_all(a).wait_send()


def put_out(*refs):
    ins, outs, sems = refs[:3], refs[3:6], refs[6]
    copies = [pltpu.make_async_copy(a, b, sems.at[k]) for k, (a, b) in enumerate(zip(ins, outs))]
    for copy in copies:
        copy.start()
    for copy in copies:
        copy.wait()


def on_device(
    right_side, positions, sphere_radii, azimuths, pair_flags, pair_counts, tilt_matrix, axial_terms
):
    vmem = pl.BlockSpec(memory_space=pltpu.VMEM)
    hbm = pl.BlockSpec(memory_space=pltpu.HBM)
    dma = pltpu.SemaphoreType.DMA
    out = jax.ShapeDtypeStruct((SD, 2, C), F32)
    V = pltpu.VMEM
    results = tuple(
        pl.pallas_call(
            kernel,
            name="bicgstab",
            out_shape=(out, out, out),
            in_specs=[hbm] * 9,
            out_specs=(vmem, vmem, vmem),
            scratch_shapes=[
                V((SD, 2, C), F32),
                V((3, SD), F32),
                V((1, SD), F32),
                V((1, SD), F32),
                V((SD, LINE * NZ * NC * SD), jnp.int32),
                V((1, SD), jnp.int32),
                V((C, C), F32),
                V((TERMS, C, C), F32),
                V((8, CP), F32),
                V((TERMS * CP, 2 * CP), BF),
                V((2 * CP, 2 * CP), BF),
                V((CP, 4 * CP), BF),
                V((NZ, SD, SRC), jnp.int32),
                V((NZ, SD, SRC), jnp.int32),
                V((8, 128), F32),
                V((8, 128), F32),
                V((8, 128), F32),
                V((LINE * NC, 8, 128), F32),
                V((NZ, 8, 128), F32),
                V((TERMS * TGT, 3 * SRC), BF),
                V((2, 2, LINE * NC, 48, 128), F32),
                V((3 * SRC, CP), BF),
                V((2 * TGT, TERMS * CP), BF),
                V((TERMS * TGT, CP), F32),
                V((TGT, CP), F32),
                V((2, 2, NZ, 48, 128), F32),
                V((2, 2, NZ, 48, 128), F32),
                V((2, SD, CP), F32),
                V((2, SD, CP), F32),
                V((2, SD, CP), F32),
                V((2, 8, 128), F32),
                V((2, NZ * NC, 8, 128), F32),
                V((2, 8, 128), F32),
                V((2, LINE, 8, 128), F32),
                dma((9,)),
                dma(()),
                dma(()),
                dma(()),
                dma(()),
                dma(()),
                dma((NZ,)),
                dma((2, 2)),
                dma((2, 2, len(RINGS))),
                dma((2, 2)),
                dma((2, 2)),
                dma((2, 2)),
                dma((2, 2)),
                dma((2,)),
                dma((2,)),
                dma((2,)),
                dma((2,)),
            ],
            compiler_params=pltpu.CompilerParams(
                collective_id=0, has_side_effects=True, vmem_limit_bytes=48 * 1024 * 1024
            ),
        )(
            *(
                pltpu.with_memory_space_constraint(x, pltpu.HBM)
                for x in (
                    right_side,
                    positions,
                    sphere_radii.reshape(1, SD),
                    azimuths.reshape(1, SD),
                    pair_flags,
                    pair_counts.reshape(1, SD),
                    tilt_matrix,
                    axial_terms,
                    jnp.asarray(orders_rows()),
                )
            )
        )
    )
    return tuple(
        pl.pallas_call(
            put_out,
            name="put_out",
            out_shape=(out, out, out),
            in_specs=[vmem] * 3,
            out_specs=(hbm,) * 3,
            scratch_shapes=[dma((3,))],
            compiler_params=pltpu.CompilerParams(vmem_limit_bytes=2 * 1024 * 1024),
        )(*results)
    )


def solution(mesh):
    split_mesh = Mesh(mesh.devices.reshape(NX, NY, NZ, NC), SPH)
    placed = (P(SPH, None, None), P(None, SPH), P(SPH), P(SPH), P(SPH, None), P(SPH), P(), P())
    return jax.shard_map(
        on_device,
        mesh=split_mesh,
        in_specs=placed,
        out_specs=(P(SPH, None, None), P(SPH, None, None), P(SPH, None, None)),
        check_vma=False,
    )
```

```python
import functools

import jax
import jax.numpy as jnp
import numpy as np
from jax import lax
from jax.experimental import pallas as pl
from jax.experimental.pallas import tpu as pltpu
from jax.sharding import Mesh
from jax.sharding import PartitionSpec as P

DEG = 12
TERMS = 8
SPH = ("sph_0", "sph_1", "sph_2", "sph_3")
NX, NY, NZ, NC = 4, 4, 8, 2
MESH = pl.DeviceIdType.MESH

coupling = 0.25
wavenum = 2.5
phase_step = 0.9
dist_floor = 0.8

SD = 16
HALF = 168
C = 336
CP = 384
LINE = NX * NY
PACKED = 42
SRC = LINE * NC * SD
TGT = NZ * SD
RINGS = (
    ((2, 2), (1, 2), (3, 2), (2, 1), (2, 3)),
    ((0, 2), (2, 0), (1, 1), (1, 3), (3, 1), (3, 3)),
    ((0, 1), (0, 3), (1, 0), (3, 0)),
)
LINE_ORDER = (4, 3, 5, 2, 6, 1, 7)
PLANE_ORDER = tuple(offset for ring in RINGS for offset in ring)
PILLAR_ORDER = tuple((j, core) for j in LINE_ORDER for core in (1, 0)) + ((0, 1),)
BF = jnp.bfloat16
F32 = jnp.float32


def orders_rows():
    orders = np.concatenate([np.arange(-degree, degree + 1) for degree in range(1, DEG + 1)])
    rows = np.zeros((8, CP), np.float32)
    rows[0, :HALF] = orders
    rows[0, HALF:C] = orders
    rows[1, :HALF] = 1.0
    rows[1, HALF:C] = -1.0
    return rows


def sincos(x):
    q = jnp.floor(x * (2.0 / np.pi) + 0.5)
    r = x - q * 1.5703125
    r = r - q * 4.83751296997070312e-4
    r = r - q * 7.54978995489188216e-8
    r2 = r * r
    s = r + r * r2 * (-1.6666654611e-1 + r2 * (8.3321608736e-3 + r2 * (-1.9515295891e-4)))
    c = 1.0 - 0.5 * r2 + r2 * r2 * (
        4.166664568298827e-2 + r2 * (-1.388731625493765e-3 + r2 * 2.443315711809948e-5)
    )
    quad = q - 4.0 * jnp.floor(q * 0.25)
    odd = (quad == 1.0) | (quad == 3.0)
    sin_sign = jnp.where(quad >= 2.0, -1.0, 1.0)
    cos_sign = jnp.where((quad == 1.0) | (quad == 2.0), -1.0, 1.0)
    return jnp.where(odd, c, s) * sin_sign, jnp.where(odd, s, c) * cos_sign


def split(x):
    high = x.astype(BF)
    return high, (x - high.astype(F32)).astype(BF)


def dot(a, b):
    return lax.dot_general(a, b, (((1,), (0,)), ((), ())), preferred_element_type=F32)


def spots():
    lane = lax.broadcasted_iota(jnp.int32, (8, 128), 1)
    row = lax.broadcasted_iota(jnp.int32, (8, 128), 0)
    return lane, row % 4


def pack(put, x):
    lane, phase = spots()
    for k in range(4):
        at = slice(8 * (k % 2), 8 * (k % 2) + 8)
        put(8 * k, x[at, 128 * (k // 2) : 128 * (k // 2) + 128])
    upper, lower = x[0:8, 256:384], x[8:16, 256:384]
    put(32, jnp.where(lane < 80, upper, pltpu.roll(lower, 80, 1)))
    rest = jnp.zeros((8, 128), F32)
    for p in range(4):
        rest = jnp.where((phase == p) & (lane // 32 == p), pltpu.roll(lower, (32 * p + 80) % 128, 1), rest)
    put(40, jnp.concatenate([jnp.sum(rest[4 * q : 4 * q + 4], axis=0, keepdims=True) for q in range(2)], axis=0))


def unpack(tiles, tail):
    lane, phase = spots()
    both = tiles[4]
    upper = jnp.where(lane < 80, both, 0.0)
    wide = jnp.concatenate([jnp.broadcast_to(tail[q : q + 1], (4, 128)) for q in range(2)], axis=0)
    rest = jnp.zeros((8, 128), F32)
    for p in range(4):
        rest = jnp.where(phase == p, pltpu.roll(wide, (48 - 32 * p) % 128, 1), rest)
    lower = jnp.where(lane < 48, pltpu.roll(both, 48, 1), jnp.where(lane < 80, rest, 0.0))
    return jnp.concatenate(
        [
            jnp.concatenate([tiles[0], tiles[1]], axis=0),
            jnp.concatenate([tiles[2], tiles[3]], axis=0),
            jnp.concatenate([upper, lower], axis=0),
        ],
        axis=1,
    )


def lanes_of(x):
    total = jnp.sum(x, axis=0, keepdims=True)
    return total[:, 0:128] + total[:, 128:256] + total[:, 256:384]


def kernel(
    vec_hbm, pos_hbm, rad_hbm, az_hbm, flags_hbm, counts_hbm, tilt_hbm, axial_hbm, rows_hbm,
    sol_ref, res_ref, dir_ref,
    vec_ref, pos_ref, rad_ref, az_ref, flags_ref, counts_ref, tilt_ref, axial, rows_ref, ax_cat, tilt_in, tilt_out, flag_out, flag_in, mine, geo_src_out, geo_tgt_out,
    geo_src, geo_tgt, w_cat, field, f_cat, g_lhs, g_acc, part, part_out, got, vec, img, img2,
    scal_out, scal_a, scal_mid, scal_b,
    in_sem, geo_src_send, geo_src_recv, geo_tgt_send, geo_tgt_recv, flag_send, flag_recv,
    field_send, field_recv, pair_send, pair_recv, part_send, part_recv,
    sa_send, sa_recv, sb_send, sb_recv,
):
    mx, my, mz, mc = (lax.axis_index(name) for name in SPH)
    plane = mx * NY + my

    def plane_peer(offset, core):
        return (lax.rem(mx + offset[0], NX), lax.rem(my + offset[1], NY), mz, core)

    def line_peer(j):
        return (mx, my, lax.rem(mz + j, NZ), mc)

    def pillar_peer(j, core):
        return (mx, my, lax.rem(mz + j, NZ), mc if core == 0 else 1 - mc)

    partner = (mx, my, mz, 1 - mc)

    def remote(src, dst, send, recv, peer):
        return pltpu.make_async_remote_copy(
            src_ref=src, dst_ref=dst, send_sem=send, recv_sem=recv, device_id=peer,
            device_id_type=MESH,
        )

    with jax.named_scope("loads"):
        pairs = (
            (pos_hbm, pos_ref), (rad_hbm, rad_ref), (az_hbm, az_ref), (counts_hbm, counts_ref),
            (rows_hbm, rows_ref), (flags_hbm, flags_ref), (tilt_hbm, tilt_ref), (vec_hbm, vec_ref),
            (axial_hbm, axial),
        )
        loads = [pltpu.make_async_copy(a, b, in_sem.at[k]) for k, (a, b) in enumerate(pairs)]
        for load in loads:
            load.start()

        barrier = pltpu.get_barrier_semaphore()

        def greet(peer):
            pl.semaphore_signal(barrier, inc=1, device_id=peer, device_id_type=MESH)

        for j, core in PILLAR_ORDER:
            greet(pillar_peer(j, core))
        for offset in PLANE_ORDER:
            for core in range(NC):
                greet(plane_peer(offset, core))

        for load in loads[:6]:
            load.wait()

    with jax.named_scope("geo_prep"):
        mine[...] = jnp.zeros((8, 128), F32)
        mine[0:3, 0:SD] = pos_ref[...]
        mine[3:4, 0:SD] = rad_ref[...]
        mine[4:5, 0:SD] = az_ref[...]
        mine[5:6, 0:SD] = counts_ref[...].astype(F32)
        own = mine[...]
        lane = lax.broadcasted_iota(jnp.int32, (8, 128), 1)
        spread = own
        for shift in (16, 32, 64):
            spread = spread + pltpu.roll(spread, shift, 1)
        geo_src_out[...] = jnp.where(lane // SD == lax.rem(plane, 8), spread, 0.0)
        geo_tgt_out[...] = jnp.where(lane // SD == mz, spread, 0.0)
        geo_src[pl.ds(plane, 1)] = geo_src_out[...][None]
        geo_tgt[pl.ds(0, 1)] = geo_tgt_out[...][None]

    with jax.named_scope("flag_prep"):
        lane = lax.broadcasted_iota(jnp.int32, (SD, 128), 1)
        for upper in range(2):
            for eight in range(2):
                sides = ([], [])
                for k in range(4):
                    at = ((8 * eight + 2 * k) * 2 + upper) * 128
                    first, second = flags_ref[:, at : at + 128], flags_ref[:, at + 256 : at + 384]
                    even = jnp.where(lane % 32 < 16, first, pltpu.roll(second, 16, 1))
                    odd = jnp.where(lane % 32 < 16, pltpu.roll(first, 112, 1), second)
                    sides[0].append(jnp.where(mc == 0, even, odd))
                    sides[1].append(jnp.where(mc == 0, odd, even))
                for side in range(2):
                    for r in range(4):
                        tile = sides[side][r]
                        for k in range(4):
                            if k != r:
                                piece = pltpu.roll(sides[side][k], (32 * (k - r)) % 128, 1)
                                tile = jnp.where(lane // 32 == k, piece, tile)
                        at = 128 * (2 * side + eight)
                        flag_out[4 * upper + r, :, at : at + 128] = tile

    with jax.named_scope("barrier_wait"):
        pl.semaphore_wait(barrier, 2 * (LINE - 1) + NZ * NC - 1)

    def src_copy(peer, other):
        to = geo_src.at[LINE * other + plane]
        return remote(geo_src_out, to, geo_src_send, geo_src_recv, peer)

    src_all_copies = remote(
        geo_src.at[pl.ds(0, LINE * NC - 1)], geo_src.at[pl.ds(0, LINE * NC - 1)],
        geo_src_send, geo_src_recv, partner,
    )

    def tgt_copy(j):
        return remote(geo_tgt_out, geo_tgt.at[j], geo_tgt_send, geo_tgt_recv, line_peer(j))

    tgt_all_copies = remote(
        geo_tgt.at[pl.ds(0, NZ - 1)], geo_tgt.at[pl.ds(0, NZ - 1)],
        geo_tgt_send, geo_tgt_recv, partner,
    )

    def flag_copy(j):
        to = lax.rem(mz + j, NZ)
        return remote(flag_out.at[to], flag_in.at[j], flag_send, flag_recv.at[j], line_peer(j))

    def blocks(a, h, count, send, recv):
        at = field.at[a, h, pl.ds(0, count), pl.ds(0, PACKED), :]
        return remote(at, at, send, recv, partner)

    def packed_block(a, h, k):
        return field.at[a, h, k, pl.ds(0, PACKED), :]

    def field_copy(a, h, ring, offset):
        at = packed_block(a, h, plane)
        return remote(at, at, field_send.at[a, h], field_recv.at[a, h, ring], plane_peer(offset, mc))

    def pair_copy(a, h, offset):
        source = lax.rem(mx + NX - offset[0], NX) * NY + lax.rem(my + NY - offset[1], NY)
        return remote(
            packed_block(a, h, source), packed_block(a, h, LINE + source), pair_send.at[a, h], pair_recv.at[a, h],
            partner,
        )

    def send_part(a, h):
        for z in range(NZ):

            def put(row, value):
                part_out[a, h, z, row : row + value.shape[0], :] = value

            pack(put, part[z * SD : (z + 1) * SD, :])
        for k, j in enumerate(LINE_ORDER):
            remote(
                part_out.at[a, h, lax.rem(mz + j, NZ), pl.ds(0, PACKED), :],
                got.at[a, h, k, pl.ds(0, PACKED), :],
                part_send.at[a, h], part_recv.at[a, h], line_peer(j),
            ).start()

    def part_all(a, h):
        at = got.at[a, h, pl.ds(0, NZ - 1), pl.ds(0, PACKED), :]
        return remote(at, at, part_send.at[a, h], part_recv.at[a, h], partner)

    def send_pillar(r):
        for k, (j, core) in enumerate(PILLAR_ORDER):
            remote(
                scal_out.at[r], scal_a.at[r, k], sa_send.at[r], sa_recv.at[r], pillar_peer(j, core)
            ).start()

    def sa_all(r):
        at = scal_a.at[r, pl.ds(0, NZ * NC - 1)]
        return remote(at, at, sa_send.at[r], sa_recv.at[r], partner)

    def send_plane(r):
        for k, offset in enumerate(PLANE_ORDER):
            remote(
                scal_mid.at[r], scal_b.at[r, k], sb_send.at[r], sb_recv.at[r],
                plane_peer(offset, mc),
            ).start()

    def sb_all(r):
        at = scal_b.at[r, pl.ds(0, LINE - 1)]
        return remote(at, at, sb_send.at[r], sb_recv.at[r], partner)

    def send_field(a, h):
        for ring, offsets in enumerate(RINGS):
            for offset in offsets:
                field_copy(a, h, ring, offset).start()
        pair_copy(a, h, (0, 0)).start()

    def relay(a, h, ring):
        with jax.named_scope(f"relay{a}{h}{ring}"):
            blocks(a, h, len(RINGS[ring]), field_send.at[a, h], field_recv.at[a, h, ring]).wait_recv()
            for offset in RINGS[ring]:
                pair_copy(a, h, offset).start()

    with jax.named_scope("sends"):
        for j in LINE_ORDER:
            tgt_copy(j).start()
        for offset in PLANE_ORDER:
            for other in range(NC):
                src_copy(plane_peer(offset, 1 - mc if other else mc), other).start()
        src_copy(partner, 1).start()
        for j in LINE_ORDER:
            flag_copy(j).start()

    loads[6].wait()
    loads[7].wait()
    cols = jnp.transpose(jnp.concatenate([own] * 16, axis=0))
    azimuth = cols[0:SD, 4:5]
    root = 1.0 / jnp.sqrt(1.0 + cols[0:SD, 5:6])
    sin_az, cos_az = sincos(azimuth * rows_ref[0:1, :])
    sin_az = sin_az * rows_ref[1:2, :]
    zeros_pad = jnp.zeros((CP - C, CP), BF)
    turned = jnp.concatenate([tilt_ref[HALF:C, :], tilt_ref[0:HALF, :]], axis=0)
    for half, block in enumerate((tilt_ref[...], turned)):
        block = jnp.concatenate([block, jnp.zeros((C, CP - C), F32)], axis=1)
        for which, value in enumerate(split(block)):
            at = slice(which * CP, (which + 1) * CP)
            tilt_in[half * CP : half * CP + C, at] = value
            tilt_in[half * CP + C : (half + 1) * CP, at] = zeros_pad

    def halves_sum(r, width):
        return r[0:SD, 0:width] + r[SD : 2 * SD, 0:width] + r[0:SD, width : 2 * width]

    def to_frame(x):
        parts = split(jnp.concatenate([x * cos_az, x * sin_az], axis=1))
        return halves_sum(dot(jnp.concatenate(parts, axis=0), tilt_in[...]), CP)

    def from_frame(x):
        u = halves_sum(dot(jnp.concatenate(split(x), axis=0), tilt_out[...]), 2 * CP)
        return (u[:, 0:CP] * cos_az + u[:, CP : 2 * CP] * sin_az) * root

    def keep(a, h, framed):
        def put(row, value):
            field[a, h, plane, row : row + value.shape[0], :] = value

        pack(put, framed)

    with jax.named_scope("frame0"):
        for h in range(2):
            v = jnp.concatenate([vec_ref[:, h, :], jnp.zeros((SD, CP - C), F32)], axis=1)
            vec[h] = v
            keep(0, h, to_frame(v))

    with jax.named_scope("send_fields"):
        send_field(0, 0)
        send_field(0, 1)

    with jax.named_scope("axial"):
        loads[8].wait()
        for m in range(TERMS):
            block = jnp.concatenate([axial[m], jnp.zeros((C, CP - C), F32)], axis=1)
            for which, value in enumerate(split(block)):
                at = slice(which * CP, (which + 1) * CP)
                ax_cat[m * CP : m * CP + C, at] = value
                ax_cat[m * CP + C : (m + 1) * CP, at] = zeros_pad
        for which in range(2):
            for half in range(2):
                at = (which * 2 + half) * CP
                tilt_out[:, at : at + CP] = jnp.transpose(
                    tilt_in[half * CP : (half + 1) * CP, which * CP : (which + 1) * CP].astype(F32)
                ).astype(BF)

    with jax.named_scope("geo_wait"):
        src_all_copies.wait_recv()
        tgt_all_copies.wait_recv()
    src_rows = []
    for tile in range(SRC // 128):
        total = geo_src[8 * tile]
        for k in range(1, 8):
            total = total + geo_src[8 * tile + k]
        src_rows.append(total)
    src_all = jnp.concatenate(src_rows, axis=1)
    tgt_all = geo_tgt[0]
    for j in range(1, NZ):
        tgt_all = tgt_all + geo_tgt[j]
    part[:, 0:128] = jnp.transpose(jnp.concatenate([tgt_all] * 16, axis=0))

    def weigh(flags, z):
        rows = pl.ds(pl.multiple_of(z * SD, SD), SD)
        tgt = part[rows, 0:128]
        dx = tgt[:, 0:1] - src_all[0:1, :]
        dy = tgt[:, 1:2] - src_all[1:2, :]
        dz = tgt[:, 2:3] - src_all[2:3, :]
        dist = jnp.sqrt(dx * dx + dy * dy + dz * dz)
        ratio = (tgt[:, 3:4] + src_all[3:4, :]) / jnp.maximum(dist, dist_floor)
        sin_d, cos_d = sincos(wavenum * dist)
        scale = jnp.where(flags != 0, coupling, 0.0)
        near = jnp.where(flags == 1, coupling, 0.0)
        for m in range(TERMS):
            if m > 0:
                near = near * ratio
                scale = near
            wave = cos_d * float(np.cos(phase_step * m)) - sin_d * float(np.sin(phase_step * m))
            high, low = split(wave * scale)
            at = pl.ds(pl.multiple_of(m * TGT + z * SD, SD), SD)
            for side in range(2):
                for k, value in enumerate((high, high, low)):
                    to = (3 * side + k) * 256
                    w_cat[at, to : to + 256] = value[:, side * 256 : (side + 1) * 256]

    with jax.named_scope("weigh"):
        weigh(flag_out[mz], mz)

        def weigh_from(k, carry):
            j = 4 + (k // 2) * (2 * lax.rem(k, 2) - 1)
            flag_copy(j).wait_recv()
            weigh(flag_in[j], lax.rem(mz + NZ - j, NZ))
            return carry

        for ring, (lo, hi) in enumerate(((1, 3), (3, 6), (6, 8))):
            relay(0, 0, ring)
            lax.fori_loop(lo, hi, weigh_from, 0)

    def reduce_pillar(r):
        with jax.named_scope(f"pillar_wait{r}"):
            sa_all(r).wait_recv()
        total = scal_out[r]
        for k in range(NZ * NC - 1):
            total = total + scal_a[r, k]
        scal_mid[r] = total
        send_plane(r)

    def reduce_plane(r):
        with jax.named_scope(f"plane_wait{r}"):
            sb_all(r).wait_recv()
        total = scal_mid[r]
        for k in range(LINE - 1):
            total = total + scal_b[r, k]
        return jnp.sum(total, axis=1, keepdims=True)

    def couple(a, h):
        def unfold(side):
            for k in range(LINE):
                tiles = [field[a, h, LINE * side + k, 8 * t : 8 * t + 8, :] for t in range(5)]
                tail = field[a, h, LINE * side + k, 40:42, :]
                high, low = split(unpack(tiles, tail))
                for t, value in enumerate((high, low, high)):
                    row = (3 * side + t) * 256 + k * SD
                    f_cat[row : row + SD, :] = value

        def arrive():
            with jax.named_scope(f"gather_wait{a}{h}"):
                blocks(a, h, LINE, pair_send.at[a, h], pair_recv.at[a, h]).wait_recv()

        split_phases = h == 0 or a == 1
        if not split_phases:
            arrive()
        with jax.named_scope(f"early{a}{h}"):
            unfold(0)
            if split_phases:
                for piece in range(2):
                    at = slice(piece * 512, (piece + 1) * 512)
                    g_acc[at, :] = dot(w_cat[at, 0:768], f_cat[0:768, :])
        if split_phases:
            arrive()
        with jax.named_scope(f"first{a}{h}"):
            unfold(1)
            for piece in range(2):
                at = slice(piece * 512, (piece + 1) * 512)
                if split_phases:
                    g = g_acc[at, :] + dot(w_cat[at, 768:1536], f_cat[768:1536, :])
                else:
                    g = dot(w_cat[at, :], f_cat[...])
                g_high, g_low = split(g)
                for k in range(4):
                    m = piece * 4 + k
                    g_lhs[0:TGT, m * CP : (m + 1) * CP] = g_high[k * TGT : (k + 1) * TGT]
                    g_lhs[TGT : 2 * TGT, m * CP : (m + 1) * CP] = g_low[k * TGT : (k + 1) * TGT]
        if h == 0 and a == 0:
            for ring in range(len(RINGS)):
                relay(0, 1, ring)
        with jax.named_scope(f"second{a}{h}"):
            both = dot(g_lhs[...], ax_cat[:, 0:CP])
            part[...] = both[0:TGT] + both[TGT : 2 * TGT] + dot(g_lhs[0:TGT, :], ax_cat[:, CP : 2 * CP])
            send_part(a, h)
        if h == 0 and a == 1:
            for ring in range(len(RINGS)):
                relay(1, 1, ring)
            reduce_pillar(0)

    def collect(a, h):
        with jax.named_scope(f"part_wait{a}{h}"):
            part_all(a, h).wait_recv()

        def summed(lo, hi):
            total = part_out[a, h, mz, lo:hi, :]
            for k in range(NZ - 1):
                total = total + got[a, h, k, lo:hi, :]
            return total

        total = unpack([summed(8 * t, 8 * t + 8) for t in range(5)], summed(40, 42))
        return from_frame(total)

    couple(0, 0)
    couple(0, 1)
    for h in range(2):
        image = vec[h] - collect(0, h)
        img[h] = image
        keep(1, h, to_frame(image))
        send_field(1, h)

    scal_out[...] = jnp.zeros((2, 8, 128), F32)
    scal_out[0, 0:1, :] = lanes_of(vec[0] * vec[0] + vec[1] * vec[1])
    scal_out[0, 1:2, :] = lanes_of(vec[0] * img[0] + vec[1] * img[1])
    send_pillar(0)
    for ring in range(len(RINGS)):
        relay(1, 0, ring)
    couple(1, 0)
    couple(1, 1)
    first_second = img[0] - collect(1, 0)
    sums = reduce_plane(0)
    rho_start = sums[0:1, :]
    alpha = rho_start / sums[1:2, :]
    right = [vec[0], vec[1]]
    half_step = [right[h] - alpha * img[h] for h in range(2)]
    half_image = [img[0] - alpha * first_second]

    def products(h):
        return (
            half_image[h] * half_step[h], half_image[h] * half_image[h],
            right[h] * half_step[h], right[h] * half_image[h],
        )

    early = [lanes_of(value) for value in products(0)]
    half_image.append(img[1] - alpha * (img[1] - collect(1, 1)))
    for row, value in enumerate(products(1)):
        scal_out[1, row : row + 1, :] = early[row] + lanes_of(value)
    send_pillar(1)
    reduce_pillar(1)
    sums = reduce_plane(1)
    omega = sums[0:1, :] / sums[1:2, :]
    rho_next = sums[2:3, :] - omega * sums[3:4, :]
    beta = rho_next / rho_start * (alpha / omega)
    for h in range(2):
        res = half_step[h] - omega * half_image[h]
        sol_ref[:, h, :] = (alpha * right[h] + omega * half_step[h])[:, 0:C]
        res_ref[:, h, :] = res[:, 0:C]
        dir_ref[:, h, :] = (res + beta * (right[h] - omega * img[h]))[:, 0:C]

    with jax.named_scope("drain"):
        src_all_copies.wait_send()
        tgt_all_copies.wait_send()
        sent = flag_in.at[pl.ds(0, NZ - 1)]
        remote(sent, sent, flag_send, flag_recv.at[0], partner).wait_send()
        for a in range(2):
            for h in range(2):
                blocks(a, h, LINE - 1, field_send.at[a, h], field_recv.at[a, h, 0]).wait_send()
                blocks(a, h, LINE, pair_send.at[a, h], pair_recv.at[a, h]).wait_send()
                part_all(a, h).wait_send()
            sa_all(a).wait_send()
            sb_all(a).wait_send()


def put_out(*refs):
    ins, outs, sems = refs[:3], refs[3:6], refs[6]
    copies = [pltpu.make_async_copy(a, b, sems.at[k]) for k, (a, b) in enumerate(zip(ins, outs))]
    for copy in copies:
        copy.start()
    for copy in copies:
        copy.wait()


def on_device(
    right_side, positions, sphere_radii, azimuths, pair_flags, pair_counts, tilt_matrix, axial_terms
):
    vmem = pl.BlockSpec(memory_space=pltpu.VMEM)
    hbm = pl.BlockSpec(memory_space=pltpu.HBM)
    dma = pltpu.SemaphoreType.DMA
    out = jax.ShapeDtypeStruct((SD, 2, C), F32)
    V = pltpu.VMEM
    results = tuple(
        pl.pallas_call(
            kernel,
            name="bicgstab",
            out_shape=(out, out, out),
            in_specs=[hbm] * 9,
            out_specs=(vmem, vmem, vmem),
            scratch_shapes=[
                V((SD, 2, C), F32),
                V((3, SD), F32),
                V((1, SD), F32),
                V((1, SD), F32),
                V((SD, LINE * NZ * NC * SD), jnp.int32),
                V((1, SD), jnp.int32),
                V((C, C), F32),
                V((TERMS, C, C), F32),
                V((8, CP), F32),
                V((TERMS * CP, 2 * CP), BF),
                V((2 * CP, 2 * CP), BF),
                V((CP, 4 * CP), BF),
                V((NZ, SD, SRC), jnp.int32),
                V((NZ, SD, SRC), jnp.int32),
                V((8, 128), F32),
                V((8, 128), F32),
                V((8, 128), F32),
                V((LINE * NC, 8, 128), F32),
                V((NZ, 8, 128), F32),
                V((TERMS * TGT, 3 * SRC), BF),
                V((2, 2, LINE * NC, 48, 128), F32),
                V((3 * SRC, CP), BF),
                V((2 * TGT, TERMS * CP), BF),
                V((TERMS * TGT, CP), F32),
                V((TGT, CP), F32),
                V((2, 2, NZ, 48, 128), F32),
                V((2, 2, NZ, 48, 128), F32),
                V((2, SD, CP), F32),
                V((2, SD, CP), F32),
                V((2, SD, CP), F32),
                V((2, 8, 128), F32),
                V((2, NZ * NC, 8, 128), F32),
                V((2, 8, 128), F32),
                V((2, LINE, 8, 128), F32),
                dma((9,)),
                dma(()),
                dma(()),
                dma(()),
                dma(()),
                dma(()),
                dma((NZ,)),
                dma((2, 2)),
                dma((2, 2, len(RINGS))),
                dma((2, 2)),
                dma((2, 2)),
                dma((2, 2)),
                dma((2, 2)),
                dma((2,)),
                dma((2,)),
                dma((2,)),
                dma((2,)),
            ],
            compiler_params=pltpu.CompilerParams(
                collective_id=0, has_side_effects=True, vmem_limit_bytes=48 * 1024 * 1024
            ),
        )(
            *(
                pltpu.with_memory_space_constraint(x, pltpu.HBM)
                for x in (
                    right_side,
                    positions,
                    sphere_radii.reshape(1, SD),
                    azimuths.reshape(1, SD),
                    pair_flags,
                    pair_counts.reshape(1, SD),
                    tilt_matrix,
                    axial_terms,
                    jnp.asarray(orders_rows()),
                )
            )
        )
    )
    return tuple(
        pl.pallas_call(
            put_out,
            name="put_out",
            out_shape=(out, out, out),
            in_specs=[vmem] * 3,
            out_specs=(hbm,) * 3,
            scratch_shapes=[dma((3,))],
            compiler_params=pltpu.CompilerParams(vmem_limit_bytes=2 * 1024 * 1024),
        )(*results)
    )


def solution(mesh):
    split_mesh = Mesh(mesh.devices.reshape(NX, NY, NZ, NC), SPH)
    placed = (P(SPH, None, None), P(None, SPH), P(SPH), P(SPH), P(SPH, None), P(SPH), P(), P())
    return jax.shard_map(
        on_device,
        mesh=split_mesh,
        in_specs=placed,
        out_specs=(P(SPH, None, None), P(SPH, None, None), P(SPH, None, None)),
        check_vma=False,
    )
```
